128 devices in a mesh: row: 16 (over y, x), col: 8 (over z, core).
Axes of the slice: x: 4, y: 4, z: 4, core: 2. Of those that a mesh axis runs over, the one named last changes fastest.
Arguments:
- field: float32 [64, 256, 1024], P(None, 'row', 'col'), may hold values from -4 to 6.5, as said below
- conductivity: float32 [64, 256, 1024], P(None, 'row', 'col'), may hold values from 35 to 5600, as said below
Outputs:
- new_field: float32 [64, 256, 1024], P(None, 'row', 'col')
The draws below stay inside these ranges and needn't reach their ends.
Inputs may be any that keep to these rules, and one draw needn't show every extreme that they name: `field`: finite values. `conductivity`: positive in every cell.
All inputs are finite; a program needn't handle non-finite values.
Results may differ from the reference program's by a relative error of at most 0.0003.
Values sent between devices are 32-bit elements; how exact they have to be, the bound alone decides.
No kernel may reach another device: no remote copies, remote signals or barrier semaphores. Data moves between devices by JAX's collectives and lax.ppermute only.
A program may use at most 64 MiB of HBM per device.

```python
import math
import jax
import jax.numpy as jnp
from jax import lax

NZ = 64
CX = 16
CY = 128
NX = 256
NY = 1024


def draw_field(key, part):
    keys = jax.random.split(jax.random.fold_in(key, 23), 5)
    x_position = (jnp.arange(NX, dtype=jnp.float32) + 0.5) / NX
    y_position = (jnp.arange(NY, dtype=jnp.float32) + 0.5) / NY
    phase_x = jax.random.uniform(keys[0], (NZ, 1, 1), jnp.float32, 0.0, 2.0 * math.pi)
    phase_y = jax.random.uniform(keys[1], (NZ, 1, 1), jnp.float32, 0.0, 2.0 * math.pi)
    noise = jnp.clip(jax.random.normal(keys[2], (NZ, NX, NY), jnp.float32), -4.0, 4.0)
    offset = jax.random.uniform(keys[3], (NZ, 1, 1), jnp.float32, 0.6, 1.5)
    amplitude = 0.5
    wave_x = jnp.sin(2.0 * math.pi * x_position[None, :, None] + phase_x)
    wave_y = jnp.sin(2.0 * math.pi * y_position[None, None, :] + phase_y)
    smooth = offset + amplitude * wave_x * wave_y
    return (noise + smooth).astype(jnp.float32)


def draw_conductivity(key, part):
    keys = jax.random.split(jax.random.fold_in(key, 11), 4)
    level = jnp.exp(jax.random.uniform(keys[0], (NZ, 1, 1), jnp.float32, math.log(200.0), math.log(4000.0)))
    x_factor = jnp.exp(jax.random.uniform(keys[1], (NZ, NX // CX, 1), jnp.float32, math.log(0.5), 0.0))
    x_factor = jnp.repeat(x_factor, CX, axis=1)
    y_factor = jnp.exp(jax.random.uniform(keys[2], (NZ, 1, NY // CY), jnp.float32, math.log(0.5), 0.0))
    y_factor = jnp.repeat(y_factor, CY, axis=2)
    rough = jnp.exp(jax.random.uniform(keys[3], (NZ, NX, NY), jnp.float32, math.log(0.7), math.log(1.4)))
    return (level * x_factor * y_factor * rough).astype(jnp.float32)


def setup_inputs(seed: int = 0) -> dict:
    streams_of = jax.random.split(jax.random.key(seed), 3)
    return {
        "field": draw_field(jax.random.fold_in(streams_of[2], 71), 0),
        "conductivity": draw_conductivity(jax.random.fold_in(streams_of[2], 71), 0),
    }


z_weight = 0.02


def neighbour(values, line_axis, offset):
    length = values.shape[line_axis]
    widths = [(0, 0)] * values.ndim
    widths[line_axis] = (1, 1)
    padded = jnp.pad(values, widths)
    return lax.slice_in_dim(padded, 1 + offset, 1 + offset + length, axis=line_axis)


def diffuse(field, conductivity, line_axis, weight):
    east_face = 0.5 * weight * (conductivity + neighbour(conductivity, line_axis, 1))
    west_face = 0.5 * weight * (conductivity + neighbour(conductivity, line_axis, -1))
    flux_here = east_face * (neighbour(field, line_axis, 1) - field) - west_face * (field - neighbour(field, line_axis, -1))
    return flux_here, west_face, east_face


def thomas(below_diag, above_diag, right_side):
    diagonal = 1.0 - below_diag - above_diag

    def forward(state_now, inputs):
        ratio_prev, value_prev = state_now
        below_here, diag_here, above_here, source_here = inputs
        pivot_here = diag_here - below_here * ratio_prev
        ratio_here = above_here / pivot_here
        value_here = (source_here - below_here * value_prev) / pivot_here
        return (ratio_here, value_here), (ratio_here, value_here)

    zero_plane = jnp.zeros_like(right_side[0])
    unused, outputs = lax.scan(forward, (zero_plane, zero_plane), (below_diag, diagonal, above_diag, right_side))

    def backward(next_value, inputs):
        ratio_here, value_here = inputs
        solved = value_here - ratio_here * next_value
        return solved, solved

    unused_last, solution = lax.scan(backward, zero_plane, outputs, reverse=True)
    return solution


def solve_lines(below_diag, above_diag, right_side, line_axis):
    solution = thomas(jnp.moveaxis(below_diag, line_axis, 0), jnp.moveaxis(above_diag, line_axis, 0), jnp.moveaxis(right_side, line_axis, 0))
    return jnp.moveaxis(solution, 0, line_axis)


def reference(field, conductivity):
    flux_zdir, west_zdir, east_zdir = diffuse(field, conductivity, 0, z_weight)
    flux_xdir, west_xdir, east_xdir = diffuse(field, conductivity, 1, 1.0)
    flux_ydir, west_ydir, east_ydir = diffuse(field, conductivity, 2, 1.0)
    explicit = flux_xdir + flux_ydir + flux_zdir
    delta_xdir = solve_lines(-west_xdir, -east_xdir, explicit, 1)
    delta_ydir = solve_lines(-west_ydir, -east_ydir, delta_xdir, 2)
    return field + delta_ydir
```

```python
import functools

import jax
import jax.numpy as jnp
from jax import lax
from jax.experimental import pallas as pl
from jax.experimental.pallas import tpu as pltpu
from jax.sharding import PartitionSpec as P

z_weight = 0.02
F32 = jnp.float32
VMEM = pl.BlockSpec(memory_space=pltpu.VMEM)
SMEM = pl.BlockSpec(memory_space=pltpu.SMEM)


def call(kernel, outs, args, flops, scratch=(), scalars=0):
    specs = [SMEM] * scalars + [VMEM] * (len(args) - scalars)
    return pl.pallas_call(
        kernel,
        out_shape=[jax.ShapeDtypeStruct(s, F32) for s in outs],
        in_specs=specs,
        out_specs=[VMEM] * len(outs),
        scratch_shapes=[pltpu.VMEM(s, F32) for s in scratch],
        cost_estimate=pl.CostEstimate(flops=flops, bytes_accessed=1 << 20, transcendentals=0),
    )(*args)


def turn(source, target, lines):
    blocks = source.shape[0] // lines
    for b in range(blocks):
        block = source[b * lines : (b + 1) * lines, :]
        target[pl.ds(b, lines, stride=blocks), :] = block.T


def edges_kernel(u, k, kt, low, high, ut):
    turn(k, kt, 128)
    turn(u, ut, 128)
    n = kt.shape[0]
    low[0:8, :] = kt[0:8, :]
    low[8:16, :] = ut[0:8, :]
    high[0:8, :] = kt[n - 8 : n, :]
    high[8:16, :] = ut[n - 8 : n, :]


def x_factor_kernel(nx, u, k, m, p, g0, gl, r):
    rows = u.shape[0]
    nz = rows // nx
    lane = lax.broadcasted_iota(jnp.int32, (nx, 128), 1)
    inner = lane < 127

    def at(ref, z):
        return ref[z * nx : (z + 1) * nx, :]

    uz, kz = at(u, 0), at(k, 0)
    below = (0.5 * z_weight) * kz * uz
    for z in range(nz):
        if z + 1 < nz:
            un, kn = at(u, z + 1), at(k, z + 1)
            above = (0.5 * z_weight) * (kz + kn) * (un - uz)
        else:
            un = kn = None
            above = -(0.5 * z_weight) * kz * uz
        flux = 0.5 * (kz + pltpu.roll(kz, 127, 1)) * (pltpu.roll(uz, 127, 1) - uz)
        flux = jnp.where(inner, flux, 0.0)
        r[z * nx : (z + 1) * nx, :] = uz + (above - below) + (flux - pltpu.roll(flux, 1, 1))
        uz, kz, below = un, kn, above

    def kx(i):
        return k[pl.ds(i, nz, stride=nx), :]

    s = jnp.ones((nz, 128), F32)
    w = s
    here = kx(0)
    for i in range(nx - 1):
        after = kx(i + 1)
        e = 0.5 * (here + after)
        inv = 1.0 / (s + e)
        mi = e * inv
        p[i] = inv
        m[i] = mi
        g0[i] = w * inv
        w = w * mi
        s = 1.0 + s * mi
        here = after
    inv = 1.0 / s
    p[nx - 1] = inv
    m[nx - 1] = jnp.zeros_like(inv)
    g = w * inv
    h = inv
    g0[nx - 1] = g
    gl[nx - 1] = h
    for i in range(nx - 2, -1, -1):
        mi = m[i]
        g = g0[i] + mi * g
        h = mi * h
        g0[i] = g
        gl[i] = h


def x_send_kernel(nx, col, low, high, from_left, from_right, r, k, g0, gl, send, rx, turned, full):
    rows = r.shape[0]
    nz = rows // nx
    first = col[0] == 0
    last = col[0] == col[1] - 1
    left = jnp.where(first, 0.0, from_left[...])
    right = jnp.where(last, 0.0, from_right[...])
    k_low, u_low = low[0:8, :], low[8:16, :]
    k_high, u_high = high[0:8, :], high[8:16, :]
    turned[0:8, :] = 0.5 * (k_low + left[0:8, :]) * (left[8:16, :] - u_low)
    turned[8:16, :] = 0.5 * (k_high + right[0:8, :]) * (right[8:16, :] - u_high)
    turned[16:128, :] = jnp.zeros((112, 128), F32)
    corr = turned[...].T
    lane = lax.broadcasted_iota(jnp.int32, (128, 128), 1)
    for b in range(rows // 128):
        west = jnp.where(lane == 0, corr[:, b : b + 1], 0.0)
        both = jnp.where(lane == 127, corr[:, 8 + b : 9 + b], west)
        full[b * 128 : (b + 1) * 128, :] = r[b * 128 : (b + 1) * 128, :] + both
    b0 = jnp.zeros((nz, 128), F32)
    bl = jnp.zeros((nz, 128), F32)
    for i in range(nx):
        ri = full[pl.ds(i, nz, stride=nx), :]
        rx[i] = ri
        b0 = b0 + g0[i] * ri
        bl = bl + gl[i] * ri
    k0 = k[pl.ds(0, nz, stride=nx), :]
    kl = k[pl.ds(nx - 1, nz, stride=nx), :]
    parts = [g0[0], g0[nx - 1], gl[nx - 1], b0, bl, k0, kl]
    peers = send.shape[0]
    own = nz // peers
    for q, part in enumerate(parts):
        for d in range(peers):
            send[d, q * own : (q + 1) * own, :] = part[d * own : (d + 1) * own, :]
    for d in range(peers):
        send[d, 7 * own : 8 * own, :] = jnp.zeros((own, 128), F32)


def x_inner_kernel(nx, rx, m, p, u, base, y):
    nz = rx.shape[1]
    v = rx[0]
    y[0] = v
    for i in range(1, nx):
        v = rx[i] + m[i - 1] * v
        y[i] = v
    b = v * p[nx - 1]
    base[nx - 1] = b - u[pl.ds(nx - 1, nz, stride=nx), :]
    for i in range(nx - 2, -1, -1):
        b = y[i] * p[i] + m[i] * b
        base[i] = b - u[pl.ds(i, nz, stride=nx), :]


def reduced(peers, take):
    zero = jnp.zeros_like(take(0)[0])
    nothing = (zero,) * 7
    before = nothing
    cp = zero
    y = zero
    cps, ys = [], []
    for i in range(peers + 1):
        after = take(i) if i < peers else nothing
        e = 0.5 * (before[6] + after[5])
        low = e * before[1]
        diag = 1.0 + e * (before[2] + after[0])
        inv = 1.0 / (diag - low * cp)
        y = (e * (after[3] - before[4]) + low * y) * inv
        cp = e * after[1] * inv
        cps.append(cp)
        ys.append(y)
        before = after
    q = ys[peers]
    out = [q]
    for i in range(peers - 1, -1, -1):
        q = ys[i] + cps[i] * q
        out.append(q)
    return out[::-1]


def x_reduced_kernel(recv, send):
    peers = recv.shape[0]
    own = recv.shape[1] // 8

    def take(d):
        return tuple(recv[d, q * own : (q + 1) * own, :] for q in range(7))

    flux = reduced(peers, take)
    for d in range(peers):
        send[d, 0:own, :] = flux[d]
        send[d, own : 2 * own, :] = flux[d + 1]


def y_factor_kernel(ny, kt, m, p, g0, gl):
    def row(ref, j):
        return ref[pl.ds(pl.multiple_of(j * 8, 8), 8), :]

    def put(ref, j, value):
        ref[pl.ds(pl.multiple_of(j * 8, 8), 8), :] = value

    one = jnp.ones((8, 128), F32)

    def forward(j, state):
        s, w, here = state
        after = row(kt, j + 1)
        e = 0.5 * (here + after)
        inv = 1.0 / (s + e)
        mi = e * inv
        put(p, j, inv)
        put(m, j, mi)
        put(g0, j, w * inv)
        return 1.0 + s * mi, w * mi, after

    s, w, unused = lax.fori_loop(0, ny - 1, forward, (one, one, row(kt, 0)))
    inv = 1.0 / s
    put(p, ny - 1, inv)
    put(m, ny - 1, jnp.zeros_like(inv))
    g = w * inv
    put(g0, ny - 1, g)
    put(gl, ny - 1, inv)

    def backward(i, state):
        g, h = state
        j = ny - 2 - i
        mi = row(m, j)
        g = row(g0, j) + mi * g
        h = mi * h
        put(g0, j, g)
        put(gl, j, h)
        return g, h

    lax.fori_loop(0, ny - 1, backward, (g, inv))


def y_send_kernel(nx, recv, base, g0x, glx, g0, gl, low, high, send, dt, ql, qr, dx):
    peers = recv.shape[0]
    own = recv.shape[1] // 2
    nz = peers * own
    for d in range(peers):
        ql[d * own : (d + 1) * own, :] = recv[d, 0:own, :]
        qr[d * own : (d + 1) * own, :] = recv[d, own : 2 * own, :]
    left, right = ql[...], qr[...]
    for i in range(nx):
        dx[pl.ds(i, nz, stride=nx), :] = base[i] + (glx[i] * right - g0x[i] * left)
    turn(dx, dt, 128)
    ny = dt.shape[0] // 8
    zero = jnp.zeros((8, 128), F32)
    b0, bl = [zero] * 4, [zero] * 4
    for j in range(ny):
        dj = dt[j * 8 : (j + 1) * 8, :]
        b0[j % 4] = b0[j % 4] + g0[j * 8 : (j + 1) * 8, :] * dj
        bl[j % 4] = bl[j % 4] + gl[j * 8 : (j + 1) * 8, :] * dj
    end = (ny - 1) * 8
    parts = [
        g0[0:8, :],
        g0[end : end + 8, :],
        gl[end : end + 8, :],
        (b0[0] + b0[1]) + (b0[2] + b0[3]),
        (bl[0] + bl[1]) + (bl[2] + bl[3]),
        low[0:8, :],
        high[0:8, :],
    ]
    for d in range(send.shape[0]):
        for q, part in enumerate(parts):
            send[d, q * 8 : (q + 1) * 8, :] = part


def y_inner_kernel(ny, dt, m, p, b, y):
    def row(ref, j):
        return ref[pl.ds(pl.multiple_of(j * 8, 8), 8), :]

    def put(ref, j, value):
        ref[pl.ds(pl.multiple_of(j * 8, 8), 8), :] = value

    put(y, 0, row(dt, 0))

    def forward(j, v):
        v = row(dt, j + 1) + row(m, j) * v
        put(y, j + 1, v)
        return v

    v = lax.fori_loop(0, ny - 1, forward, row(dt, 0), unroll=8)
    v = v * row(p, ny - 1)
    put(b, ny - 1, v)

    def backward(i, v):
        j = ny - 2 - i
        v = row(y, j) * row(p, j) + row(m, j) * v
        put(b, j, v)
        return v

    lax.fori_loop(0, ny - 1, backward, v, unroll=8)


def finish_kernel(col, recv, b, g0, gl, u, out, flux, whole):
    peers = recv.shape[0]

    def take(d):
        return tuple(recv[d, q * 8 : (q + 1) * 8, :] for q in range(7))

    q = reduced(peers, take)
    for i in range(peers + 1):
        flux[i] = q[i]
    left = flux[col[0]]
    right = flux[col[0] + 1]
    ny = b.shape[0] // 8
    for j in range(ny):
        sl = slice(j * 8, (j + 1) * 8)
        whole[sl, :] = b[sl, :] + (gl[sl, :] * right - g0[sl, :] * left)
    for i in range(8):
        rows = slice(i * 128, (i + 1) * 128)
        out[rows, :] = u[rows, :] + whole[pl.ds(i, 128, stride=8), :].T


def on_device(field, conductivity):
    nz, nx, ny = field.shape
    rows = nz * nx
    rowp, colp = lax.axis_size("row"), lax.axis_size("col")
    own = nz // rowp
    u = field.reshape(rows, ny)
    k = conductivity.reshape(rows, ny)
    col = jnp.stack([lax.axis_index("col"), jnp.int32(colp)]).astype(jnp.int32)
    flat, cube = (rows, ny), (nx, nz, ny)
    kt, low, high = call(edges_kernel, [flat, (16, 128), (16, 128)], (u, k), 1 << 20, [flat])
    up = [(i, (i + 1) % colp) for i in range(colp)]
    from_left = lax.ppermute(high, "col", up)
    from_right = lax.ppermute(low, "col", [(b, a) for a, b in up])
    m, p, g0, gl, r = call(
        functools.partial(x_factor_kernel, nx), [cube] * 4 + [flat], (u, k), 1 << 23
    )
    send, rx = call(
        functools.partial(x_send_kernel, nx),
        [(rowp, 8 * own, ny), cube],
        (col, low, high, from_left, from_right, r, k, g0, gl),
        1 << 22,
        [(128, 128), flat],
        1,
    )
    recv = lax.all_to_all(send, "row", 0, 0, tiled=True)
    (base,) = call(functools.partial(x_inner_kernel, nx), [cube], (rx, m, p, u), 1 << 22, [cube])
    my, py, g0y, gly = call(functools.partial(y_factor_kernel, ny), [flat] * 4, (kt,), 1 << 23)
    (back,) = call(x_reduced_kernel, [(rowp, 2 * own, ny)], (recv,), 1 << 21)
    recv = lax.all_to_all(back, "row", 0, 0, tiled=True)
    send, dt = call(
        functools.partial(y_send_kernel, nx),
        [(colp, 56, 128), flat],
        (recv, base, g0, gl, g0y, gly, low, high),
        1 << 22,
        [(nz, ny), (nz, ny), flat],
    )
    recv = lax.all_to_all(send, "col", 0, 0, tiled=True)
    (b,) = call(functools.partial(y_inner_kernel, ny), [flat], (dt, my, py), 1 << 22, [flat])
    (out,) = call(
        finish_kernel, [flat], (col, recv, b, g0y, gly, u), 1 << 22, [(colp + 1, 8, 128), flat], 1
    )
    return out.reshape(nz, nx, ny)


def solution(mesh):
    in_specs = (P(None, "row", "col"), P(None, "row", "col"))
    out_specs = P(None, "row", "col")
    return jax.shard_map(
        on_device, mesh=mesh, in_specs=in_specs, out_specs=out_specs, check_vma=False
    )
```

```python
import functools

import jax
import jax.numpy as jnp
from jax import lax
from jax.experimental import pallas as pl
from jax.experimental.pallas import tpu as pltpu
from jax.sharding import PartitionSpec as P

z_weight = 0.02
F32 = jnp.float32
VMEM = pl.BlockSpec(memory_space=pltpu.VMEM)
HBM = pl.BlockSpec(memory_space=pltpu.HBM)
CHUNKS = 4


def call(kernel, outs, args, flops, scratch=(), specs=None):
    return pl.pallas_call(
        kernel,
        out_shape=[jax.ShapeDtypeStruct(s, F32) for s in outs],
        in_specs=specs or [VMEM] * len(args),
        out_specs=[VMEM] * len(outs),
        scratch_shapes=[pltpu.VMEM(s, F32) if isinstance(s, tuple) else s for s in scratch],
        compiler_params=pltpu.CompilerParams(vmem_limit_bytes=12 << 20),
        cost_estimate=pl.CostEstimate(flops=flops, bytes_accessed=1 << 20, transcendentals=0),
    )(*args)


def row(ref, j):
    start = j * 8 if isinstance(j, int) else pl.multiple_of(j * 8, 8)
    return ref[pl.ds(start, 8), :]


def put(ref, j, value):
    start = j * 8 if isinstance(j, int) else pl.multiple_of(j * 8, 8)
    ref[pl.ds(start, 8), :] = value


def turn(source, target, b):
    target[pl.ds(b, 128, stride=8), :] = source[b * 128 : (b + 1) * 128, :].T


def turn_back(source, b):
    return source[pl.ds(b, 128, stride=8), :].T


def load_kernel(u_hbm, k_hbm, u, k, ut, kt, low, high, sems):
    rows = u.shape[0] // CHUNKS
    copies = []
    for c in range(CHUNKS):
        part = pl.ds(c * rows, rows)
        for a, (src, dst) in enumerate(((k_hbm, k), (u_hbm, u))):
            copy = pltpu.make_async_copy(src.at[part], dst.at[part], sems.at[2 * c + a])
            copy.start()
            copies.append(copy)
    for c in range(CHUNKS):
        for a, (src, dst) in enumerate(((k, kt), (u, ut))):
            copies[2 * c + a].wait()
            for b in range(c * rows // 128, (c + 1) * rows // 128):
                turn(src, dst, b)
    n = kt.shape[0] // 8
    low[0:8, :] = row(kt, 0)
    low[8:16, :] = row(ut, 0)
    high[0:8, :] = row(kt, n - 1)
    high[8:16, :] = row(ut, n - 1)


def pivots_kernel(nx, u, k, ut, kt, mx, px, r, ends, my, py, lt):
    rows = u.shape[0]
    nz = rows // nx
    ny = lt.shape[0] // 8
    half = ny // 2

    def both(i, state):
        s, t, k_left, k_right = state
        j = ny - 1 - i
        next_left, next_right = row(kt, i + 1), row(kt, j - 1)
        e = 0.5 * (k_left + next_left)
        f = 0.5 * (k_right + next_right)
        inv_e = 1.0 / (s + e)
        inv_f = 1.0 / (t + f)
        m_left, m_right = e * inv_e, f * inv_f
        put(py, i, inv_e)
        put(py, j, inv_f)
        put(my, i, m_left)
        put(my, j, m_right)
        return 1.0 + s * m_left, 1.0 + t * m_right, next_left, next_right

    one = jnp.ones((8, 128), F32)
    s, t, k_left, k_right = lax.fori_loop(
        0, half - 1, both, (one, one, row(kt, 0), row(kt, ny - 1)), unroll=7
    )
    e = 0.5 * (k_left + k_right)
    inv = 1.0 / (s * t + e * (s + t))
    put(py, half - 1, (t + e) * inv)
    put(py, half, (s + e) * inv)
    put(my, half - 1, e * inv)
    put(my, half, e * inv)

    here_k, here_u = row(kt, 0), row(ut, 0)
    before = None
    for j in range(ny):
        if j + 1 < ny:
            next_k, next_u = row(kt, j + 1), row(ut, j + 1)
            flux = 0.5 * (here_k + next_k) * (next_u - here_u)
            put(lt, j, flux if before is None else flux - before)
            before, here_k, here_u = flux, next_k, next_u
        else:
            put(lt, j, -before)

    def at(ref, z):
        return ref[z * nx : (z + 1) * nx, :]

    uz, kz = at(u, 0), at(k, 0)
    below = (0.5 * z_weight) * kz * uz
    side = None
    for z in range(nz):
        if z * nx % 128 == 0:
            side = turn_back(lt, z * nx // 128)
        if z + 1 < nz:
            un, kn = at(u, z + 1), at(k, z + 1)
            above = (0.5 * z_weight) * (kz + kn) * (un - uz)
        else:
            un = kn = None
            above = -(0.5 * z_weight) * kz * uz
        part = z * nx % 128
        r[z * nx : (z + 1) * nx, :] = uz + (above - below) + side[part : part + nx, :]
        uz, kz, below = un, kn, above

    def kx(i):
        return k[pl.ds(i, nz, stride=nx), :]

    s = jnp.ones((nz, 128), F32)
    here = kx(0)
    ends[0] = here
    for i in range(nx - 1):
        after = kx(i + 1)
        e = 0.5 * (here + after)
        inv = 1.0 / (s + e)
        m = e * inv
        px[i] = inv
        mx[i] = m
        s = 1.0 + s * m
        here = after
    px[nx - 1] = 1.0 / s
    ends[1] = here


def x_send_kernel(nx, peers_y, low, high, from_left, from_right, r, ends, m, p, send, b, g0, gl, turned, full):
    rows = r.shape[0]
    nz = rows // nx
    col = lax.axis_index("col")
    left = jnp.where(col == 0, 0.0, from_left[...])
    right = jnp.where(col == peers_y - 1, 0.0, from_right[...])
    k_low, u_low = low[0:8, :], low[8:16, :]
    k_high, u_high = high[0:8, :], high[8:16, :]
    turned[0:8, :] = 0.5 * (k_low + left[0:8, :]) * (left[8:16, :] - u_low)
    turned[8:16, :] = 0.5 * (k_high + right[0:8, :]) * (right[8:16, :] - u_high)
    turned[16:128, :] = jnp.zeros((112, 128), F32)
    corr = turned[...].T
    lane = lax.broadcasted_iota(jnp.int32, (128, 128), 1)
    for i in range(rows // 128):
        west = jnp.where(lane == 0, corr[:, i : i + 1], 0.0)
        both = jnp.where(lane == 127, corr[:, 8 + i : 9 + i], west)
        full[i * 128 : (i + 1) * 128, :] = r[i * 128 : (i + 1) * 128, :] + both
    y = full[pl.ds(0, nz, stride=nx), :]
    w = jnp.ones((nz, 128), F32)
    for i in range(nx - 1):
        mi, pi = m[i], p[i]
        b[i] = y * pi
        g0[i] = w * pi
        y = full[pl.ds(i + 1, nz, stride=nx), :] + mi * y
        w = w * mi
    h = p[nx - 1]
    v = y * h
    g = w * h
    b[nx - 1] = v
    g0[nx - 1] = g
    gl[nx - 1] = h
    parts = [None, g, h, None, v, ends[0], ends[1]]
    for i in range(nx - 2, -1, -1):
        mi = m[i]
        v = b[i] + mi * v
        g = g0[i] + mi * g
        h = mi * h
        b[i] = v
        g0[i] = g
        gl[i] = h
    parts[0] = g
    parts[3] = v
    peers = send.shape[0]
    own = nz // peers
    for q, part in enumerate(parts):
        for d in range(peers):
            send[d, q * own : (q + 1) * own, :] = part[d * own : (d + 1) * own, :]
    for d in range(peers):
        send[d, 7 * own : 8 * own, :] = jnp.zeros((own, 128), F32)


def reduced(peers, take):
    zero = jnp.zeros_like(take(0)[0])
    nothing = (zero,) * 7
    before = nothing
    cp = zero
    y = zero
    cps, ys = [], []
    for i in range(peers + 1):
        after = take(i) if i < peers else nothing
        e = 0.5 * (before[6] + after[5])
        low = e * before[1]
        diag = 1.0 + e * (before[2] + after[0])
        inv = 1.0 / (diag - low * cp)
        y = (e * (after[3] - before[4]) + low * y) * inv
        cp = e * after[1] * inv
        cps.append(cp)
        ys.append(y)
        before = after
    q = ys[peers]
    out = [q]
    for i in range(peers - 1, -1, -1):
        q = ys[i] + cps[i] * q
        out.append(q)
    return out[::-1]


def x_reduced_kernel(recv, send):
    peers = recv.shape[0]
    own = recv.shape[1] // 8

    def take(d):
        return tuple(recv[d, q * own : (q + 1) * own, :] for q in range(7))

    flux = reduced(peers, take)
    for d in range(peers):
        send[d, 0:own, :] = flux[d]
        send[d, own : 2 * own, :] = flux[d + 1]


def y_send_kernel(nx, recv, bx, g0x, glx, u, m, p, low, high, send, b, g0, gl, dt, ql, qr, dx):
    peers = recv.shape[0]
    own = recv.shape[1] // 2
    nz = peers * own
    ny = dt.shape[0] // 8
    half = ny // 2
    for d in range(peers):
        ql[d * own : (d + 1) * own, :] = recv[d, 0:own, :]
        qr[d * own : (d + 1) * own, :] = recv[d, own : 2 * own, :]
    left, right = ql[...], qr[...]
    for i in range(nx):
        part = pl.ds(i, nz, stride=nx)
        dx[part, :] = (bx[i] - u[part, :]) + (glx[i] * right - g0x[i] * left)
    for i in range(8):
        turn(dx, dt, i)

    def forward(i, state):
        y, w, z, x = state
        j = ny - 1 - i
        m_left, p_left = row(m, i), row(p, i)
        m_right, p_right = row(m, j), row(p, j)
        put(b, i, y * p_left)
        put(g0, i, w * p_left)
        put(b, j, z * p_right)
        put(gl, j, x * p_right)
        return (
            row(dt, i + 1) + m_left * y,
            w * m_left,
            row(dt, j - 1) + m_right * z,
            x * m_right,
        )

    one = jnp.ones((8, 128), F32)
    y, w, z, x = lax.fori_loop(
        0, half - 1, forward, (row(dt, 0), one, row(dt, ny - 1), one), unroll=7
    )
    c_left, c_right, c_mid = row(p, half - 1), row(p, half), row(m, half)
    state = (
        c_left * y + c_mid * z,
        c_left * w,
        c_mid * x,
        c_right * z + c_mid * y,
        c_mid * w,
        c_right * x,
    )

    def save(i, j, state):
        put(b, i, state[0])
        put(g0, i, state[1])
        put(gl, i, state[2])
        put(b, j, state[3])
        put(g0, j, state[4])
        put(gl, j, state[5])

    save(half - 1, half, state)

    def backward(n, state):
        i = half - 2 - n
        j = ny - 1 - i
        m_left, m_right = row(m, i), row(m, j)
        state = (
            row(b, i) + m_left * state[0],
            row(g0, i) + m_left * state[1],
            m_left * state[2],
            row(b, j) + m_right * state[3],
            m_right * state[4],
            row(gl, j) + m_right * state[5],
        )
        save(i, j, state)
        return state

    state = lax.fori_loop(0, half - 1, backward, state, unroll=7)
    parts = [state[1], state[4], state[5], state[0], state[3], low[0:8, :], high[0:8, :]]
    for d in range(send.shape[0]):
        for q, part in enumerate(parts):
            send[d, q * 8 : (q + 1) * 8, :] = part


def finish_kernel(recv, b, g0, gl, u, out, flux, whole):
    peers = recv.shape[0]

    def take(d):
        return tuple(recv[d, q * 8 : (q + 1) * 8, :] for q in range(7))

    q = reduced(peers, take)
    for i in range(peers + 1):
        flux[i] = q[i]
    col = lax.axis_index("col")
    left = flux[col]
    right = flux[col + 1]
    for j in range(b.shape[0] // 8):
        put(whole, j, row(b, j) + (row(gl, j) * right - row(g0, j) * left))
    for i in range(8):
        rows = slice(i * 128, (i + 1) * 128)
        out[rows, :] = u[rows, :] + turn_back(whole, i)


def on_device(field, conductivity):
    nz, nx, ny = field.shape
    rows = nz * nx
    rowp, colp = lax.axis_size("row"), lax.axis_size("col")
    own = nz // rowp
    u = field.reshape(rows, ny)
    k = conductivity.reshape(rows, ny)
    flat, cube = (rows, ny), (nx, nz, ny)
    uv, kv, ut, kt, low, high = call(
        load_kernel,
        [flat] * 4 + [(16, 128)] * 2,
        tuple(pltpu.with_memory_space_constraint(a, pltpu.HBM) for a in (u, k)),
        1 << 20,
        [pltpu.SemaphoreType.DMA((2 * CHUNKS,))],
        [HBM, HBM],
    )
    up = [(i, (i + 1) % colp) for i in range(colp)]
    from_left = lax.ppermute(high, "col", up)
    from_right = lax.ppermute(low, "col", [(b, a) for a, b in up])
    mx, px, r, ends, my, py = call(
        functools.partial(pivots_kernel, nx),
        [cube] * 2 + [flat, (2, nz, ny)] + [flat] * 2,
        (uv, kv, ut, kt),
        1 << 23,
        [flat],
    )
    send, bx, g0x, glx = call(
        functools.partial(x_send_kernel, nx, colp),
        [(rowp, 8 * own, ny)] + [cube] * 3,
        (low, high, from_left, from_right, r, ends, mx, px),
        1 << 22,
        [(128, 128), flat],
    )
    recv = lax.all_to_all(send, "row", 0, 0, tiled=True)
    (back,) = call(x_reduced_kernel, [(rowp, 2 * own, ny)], (recv,), 1 << 21)
    recv = lax.all_to_all(back, "row", 0, 0, tiled=True)
    send, b, g0y, gly = call(
        functools.partial(y_send_kernel, nx),
        [(colp, 56, 128)] + [flat] * 3,
        (recv, bx, g0x, glx, u, my, py, low, high),
        1 << 22,
        [flat, (nz, ny), (nz, ny), flat],
    )
    recv = lax.all_to_all(send, "col", 0, 0, tiled=True)
    (out,) = call(
        finish_kernel, [flat], (recv, b, g0y, gly, u), 1 << 22, [(colp + 1, 8, 128), flat]
    )
    return out.reshape(nz, nx, ny)


def solution(mesh):
    in_specs = (P(None, "row", "col"), P(None, "row", "col"))
    out_specs = P(None, "row", "col")
    return jax.shard_map(
        on_device, mesh=mesh, in_specs=in_specs, out_specs=out_specs, check_vma=False
    )
```

```python
import functools

import jax
import jax.numpy as jnp
from jax import lax
from jax.experimental import pallas as pl
from jax.experimental.pallas import tpu as pltpu
from jax.sharding import PartitionSpec as P

z_weight = 0.02
F32 = jnp.float32
VMEM = pl.BlockSpec(memory_space=pltpu.VMEM)
HBM = pl.BlockSpec(memory_space=pltpu.HBM)
CHUNKS = 4


def call(kernel, outs, args, flops, scratch=(), specs=None, out_specs=None):
    return pl.pallas_call(
        kernel,
        out_shape=[jax.ShapeDtypeStruct(s, F32) for s in outs],
        in_specs=specs or [VMEM] * len(args),
        out_specs=out_specs or [VMEM] * len(outs),
        scratch_shapes=[pltpu.VMEM(s, F32) if isinstance(s, tuple) else s for s in scratch],
        compiler_params=pltpu.CompilerParams(vmem_limit_bytes=12 << 20),
        cost_estimate=pl.CostEstimate(flops=flops, bytes_accessed=1 << 20, transcendentals=0),
    )(*args)


def row(ref, j):
    start = j * 8 if isinstance(j, int) else pl.multiple_of(j * 8, 8)
    return ref[pl.ds(start, 8), :]


def put(ref, j, value):
    start = j * 8 if isinstance(j, int) else pl.multiple_of(j * 8, 8)
    ref[pl.ds(start, 8), :] = value


def turn(source, target, b):
    target[pl.ds(b, 128, stride=8), :] = source[b * 128 : (b + 1) * 128, :].T


def turn_back(source, b):
    return source[pl.ds(b, 128, stride=8), :].T


def load_kernel(u_hbm, k_hbm, u, k, ut, kt, low, high, sems):
    rows = u.shape[0] // CHUNKS
    copies = []
    for c in range(CHUNKS):
        part = pl.ds(c * rows, rows)
        for a, (src, dst) in enumerate(((k_hbm, k), (u_hbm, u))):
            copy = pltpu.make_async_copy(src.at[part], dst.at[part], sems.at[2 * c + a])
            copy.start()
            copies.append(copy)
    for c in range(CHUNKS):
        for a, (src, dst) in enumerate(((k, kt), (u, ut))):
            copies[2 * c + a].wait()
            for b in range(c * rows // 128, (c + 1) * rows // 128):
                turn(src, dst, b)
    n = kt.shape[0] // 8
    low[0:8, :] = row(kt, 0)
    low[8:16, :] = row(ut, 0)
    high[0:8, :] = row(kt, n - 1)
    high[8:16, :] = row(ut, n - 1)


def pivots_kernel(nx, u, k, ut, kt, mx, px, r, ends, my, py, lt):
    rows = u.shape[0]
    nz = rows // nx
    ny = lt.shape[0] // 8
    half = ny // 2

    def both(i, state):
        s, t, k_left, k_right = state
        j = ny - 1 - i
        next_left, next_right = row(kt, i + 1), row(kt, j - 1)
        e = 0.5 * (k_left + next_left)
        f = 0.5 * (k_right + next_right)
        inv_e = 1.0 / (s + e)
        inv_f = 1.0 / (t + f)
        m_left, m_right = e * inv_e, f * inv_f
        put(py, i, inv_e)
        put(py, j, inv_f)
        put(my, i, m_left)
        put(my, j, m_right)
        return 1.0 + s * m_left, 1.0 + t * m_right, next_left, next_right

    one = jnp.ones((8, 128), F32)
    s, t, k_left, k_right = lax.fori_loop(
        0, half - 1, both, (one, one, row(kt, 0), row(kt, ny - 1)), unroll=7
    )
    e = 0.5 * (k_left + k_right)
    inv = 1.0 / (s * t + e * (s + t))
    put(py, half - 1, (t + e) * inv)
    put(py, half, (s + e) * inv)
    put(my, half - 1, e * inv)
    put(my, half, e * inv)

    here_k, here_u = row(kt, 0), row(ut, 0)
    before = None
    for j in range(ny):
        if j + 1 < ny:
            next_k, next_u = row(kt, j + 1), row(ut, j + 1)
            flux = 0.5 * (here_k + next_k) * (next_u - here_u)
            put(lt, j, flux if before is None else flux - before)
            before, here_k, here_u = flux, next_k, next_u
        else:
            put(lt, j, -before)

    def at(ref, z):
        return ref[z * nx : (z + 1) * nx, :]

    uz, kz = at(u, 0), at(k, 0)
    below = (0.5 * z_weight) * kz * uz
    side = None
    for z in range(nz):
        if z * nx % 128 == 0:
            side = turn_back(lt, z * nx // 128)
        if z + 1 < nz:
            un, kn = at(u, z + 1), at(k, z + 1)
            above = (0.5 * z_weight) * (kz + kn) * (un - uz)
        else:
            un = kn = None
            above = -(0.5 * z_weight) * kz * uz
        part = z * nx % 128
        r[z * nx : (z + 1) * nx, :] = uz + (above - below) + side[part : part + nx, :]
        uz, kz, below = un, kn, above

    def kx(i):
        return k[pl.ds(i, nz, stride=nx), :]

    s = jnp.ones((nz, 128), F32)
    here = kx(0)
    ends[0] = here
    for i in range(nx - 1):
        after = kx(i + 1)
        e = 0.5 * (here + after)
        inv = 1.0 / (s + e)
        m = e * inv
        px[i] = inv
        mx[i] = m
        s = 1.0 + s * m
        here = after
    px[nx - 1] = 1.0 / s
    ends[1] = here


def x_send_kernel(nx, peers_y, low, high, from_left, from_right, r, ends, m, p, send, b, g0, gl, faces, turned, full):
    rows = r.shape[0]
    nz = rows // nx
    col = lax.axis_index("col")
    left = jnp.where(col == 0, 0.0, from_left[...])
    right = jnp.where(col == peers_y - 1, 0.0, from_right[...])
    k_low, u_low = low[0:8, :], low[8:16, :]
    k_high, u_high = high[0:8, :], high[8:16, :]
    face_left = 0.5 * (k_low + left[0:8, :])
    face_right = 0.5 * (k_high + right[0:8, :])
    faces[0:8, :] = jnp.sqrt(face_left)
    faces[8:16, :] = jnp.sqrt(face_right)
    turned[0:8, :] = face_left * (left[8:16, :] - u_low)
    turned[8:16, :] = face_right * (right[8:16, :] - u_high)
    turned[16:128, :] = jnp.zeros((112, 128), F32)
    corr = turned[...].T
    lane = lax.broadcasted_iota(jnp.int32, (128, 128), 1)
    for i in range(rows // 128):
        west = jnp.where(lane == 0, corr[:, i : i + 1], 0.0)
        both = jnp.where(lane == 127, corr[:, 8 + i : 9 + i], west)
        full[i * 128 : (i + 1) * 128, :] = r[i * 128 : (i + 1) * 128, :] + both
    y = full[pl.ds(0, nz, stride=nx), :]
    w = jnp.ones((nz, 128), F32)
    for i in range(nx - 1):
        mi, pi = m[i], p[i]
        b[i] = y * pi
        g0[i] = w * pi
        y = full[pl.ds(i + 1, nz, stride=nx), :] + mi * y
        w = w * mi
    h = p[nx - 1]
    v = y * h
    g = w * h
    b[nx - 1] = v
    g0[nx - 1] = g
    gl[nx - 1] = h
    parts = [None, g, h, None, v, ends[0], ends[1]]
    for i in range(nx - 2, -1, -1):
        mi = m[i]
        v = b[i] + mi * v
        g = g0[i] + mi * g
        h = mi * h
        b[i] = v
        g0[i] = g
        gl[i] = h
    parts[0] = g
    parts[3] = v
    peers = send.shape[0]
    own = nz // peers
    for q, part in enumerate(parts):
        for d in range(peers):
            send[d, q * own : (q + 1) * own, :] = part[d * own : (d + 1) * own, :]
    for d in range(peers):
        send[d, 7 * own : 8 * own, :] = jnp.zeros((own, 128), F32)


def solve(low, diag, up, rhs):
    n = len(diag)
    mid = n // 2
    c, q = [None] * n, [None] * n
    for order, near, far in (
        (range(mid), low, up),
        (range(n - 1, mid, -1), up, low),
    ):
        last = None
        for i in order:
            if last is None:
                inv = 1.0 / diag[i]
                q[i] = rhs[i] * inv
            else:
                inv = 1.0 / (diag[i] - near[i] * c[last])
                q[i] = (rhs[i] + near[i] * q[last]) * inv
            c[i] = far[i] * inv
            last = i
    i = mid
    inv = 1.0 / (diag[i] - low[i] * c[i - 1] - up[i] * c[i + 1])
    q[i] = (rhs[i] + low[i] * q[i - 1] + up[i] * q[i + 1]) * inv
    for i in range(mid - 1, -1, -1):
        q[i] = q[i] + c[i] * q[i + 1]
    for i in range(mid + 1, n):
        q[i] = q[i] + c[i] * q[i - 1]
    return q


def x_reduced_kernel(recv, send):
    peers = recv.shape[0]
    own = recv.shape[1] // 8
    nothing = (jnp.zeros((own, 128), F32),) * 7
    low, diag, up, rhs = [], [], [], []
    before = nothing
    for i in range(peers + 1):
        after = nothing
        if i < peers:
            after = tuple(recv[i, q * own : (q + 1) * own, :] for q in range(7))
        e = 0.5 * (before[6] + after[5])
        low.append(e * before[1])
        diag.append(1.0 + e * (before[2] + after[0]))
        up.append(e * after[1])
        rhs.append(e * (after[3] - before[4]))
        before = after
    flux = solve(low, diag, up, rhs)
    for d in range(peers):
        send[d, 0:own, :] = flux[d]
        send[d, own : 2 * own, :] = flux[d + 1]


def y_send_kernel(nx, recv, bx, g0x, glx, u, m, p, faces, send, b, g0, gl, dt, ql, qr, dx):
    peers = recv.shape[0]
    own = recv.shape[1] // 2
    nz = peers * own
    ny = dt.shape[0] // 8
    half = ny // 2
    for d in range(peers):
        ql[d * own : (d + 1) * own, :] = recv[d, 0:own, :]
        qr[d * own : (d + 1) * own, :] = recv[d, own : 2 * own, :]
    left, right = ql[...], qr[...]
    for i in range(nx):
        part = pl.ds(i, nz, stride=nx)
        dx[part, :] = (bx[i] - u[part, :]) + (glx[i] * right - g0x[i] * left)
    for i in range(8):
        turn(dx, dt, i)

    w = x = jnp.ones((8, 128), F32)
    y, z = row(dt, 0), row(dt, ny - 1)
    for i in range(half - 1):
        j = ny - 1 - i
        m_left, p_left = row(m, i), row(p, i)
        m_right, p_right = row(m, j), row(p, j)
        put(b, i, y * p_left)
        put(g0, i, w * p_left)
        put(b, j, z * p_right)
        put(gl, j, x * p_right)
        y = row(dt, i + 1) + m_left * y
        w = w * m_left
        z = row(dt, j - 1) + m_right * z
        x = x * m_right
    c_left, c_right, c_mid = row(p, half - 1), row(p, half), row(m, half)
    b_left, b_right = c_left * y + c_mid * z, c_right * z + c_mid * y
    g_left, g_right = c_left * w, c_mid * w
    h_left, h_right = c_mid * x, c_right * x
    for i in range(half - 1, -1, -1):
        j = ny - 1 - i
        if i < half - 1:
            m_left, m_right = row(m, i), row(m, j)
            b_left = row(b, i) + m_left * b_left
            g_left = row(g0, i) + m_left * g_left
            h_left = m_left * h_left
            b_right = row(b, j) + m_right * b_right
            g_right = m_right * g_right
            h_right = row(gl, j) + m_right * h_right
        put(b, i, b_left)
        put(g0, i, g_left)
        put(gl, i, h_left)
        put(b, j, b_right)
        put(g0, j, g_right)
        put(gl, j, h_right)
    root_left, root_right = faces[0:8, :], faces[8:16, :]
    parts = [
        root_left * root_left * g_left,
        root_left * root_right * g_right,
        root_right * root_right * h_right,
        root_left * b_left,
        root_right * b_right,
    ]
    for d in range(send.shape[0]):
        for q, part in enumerate(parts):
            send[d, q * 8 : (q + 1) * 8, :] = part


def finish_kernel(recv, b, g0, gl, u, faces, out, flux, done, sems):
    peers = recv.shape[0]
    nothing = (jnp.zeros((8, 128), F32),) * 5
    low, diag, up, rhs = [], [], [], []
    before = nothing
    for i in range(peers + 1):
        after = nothing
        if i < peers:
            after = tuple(recv[i, q * 8 : (q + 1) * 8, :] for q in range(5))
        low.append(before[1])
        diag.append(1.0 + (before[2] + after[0]))
        up.append(after[1])
        rhs.append(after[3] - before[4])
        before = after
    q = solve(low, diag, up, rhs)
    for i in range(peers + 1):
        flux[i] = q[i]
    col = lax.axis_index("col")
    left = flux[col] * faces[0:8, :]
    right = flux[col + 1] * faces[8:16, :]
    copies = []
    for i in range(8):
        part = pl.ds(i, 128, stride=8)
        delta = b[part, :] + (gl[part, :] * right[i : i + 1, :] - g0[part, :] * left[i : i + 1, :])
        rows = pl.ds(i * 128, 128)
        done[rows, :] = u[rows, :] + delta.T
        copy = pltpu.make_async_copy(done.at[rows], out.at[rows], sems.at[i])
        copy.start()
        copies.append(copy)
    for copy in copies:
        copy.wait()


def on_device(field, conductivity):
    nz, nx, ny = field.shape
    rows = nz * nx
    rowp, colp = lax.axis_size("row"), lax.axis_size("col")
    own = nz // rowp
    u = field.reshape(rows, ny)
    k = conductivity.reshape(rows, ny)
    flat, cube = (rows, ny), (nx, nz, ny)
    uv, kv, ut, kt, low, high = call(
        load_kernel,
        [flat] * 4 + [(16, 128)] * 2,
        tuple(pltpu.with_memory_space_constraint(a, pltpu.HBM) for a in (u, k)),
        1 << 20,
        [pltpu.SemaphoreType.DMA((2 * CHUNKS,))],
        [HBM, HBM],
    )
    up = [(i, (i + 1) % colp) for i in range(colp)]
    from_left = lax.ppermute(high, "col", up)
    from_right = lax.ppermute(low, "col", [(b, a) for a, b in up])
    mx, px, r, ends, my, py = call(
        functools.partial(pivots_kernel, nx),
        [cube] * 2 + [flat, (2, nz, ny)] + [flat] * 2,
        (uv, kv, ut, kt),
        1 << 23,
        [flat],
    )
    send, bx, g0x, glx, faces = call(
        functools.partial(x_send_kernel, nx, colp),
        [(rowp, 8 * own, ny)] + [cube] * 3 + [(16, 128)],
        (low, high, from_left, from_right, r, ends, mx, px),
        1 << 22,
        [(128, 128), flat],
    )
    recv = lax.all_to_all(send, "row", 0, 0, tiled=True)
    (back,) = call(x_reduced_kernel, [(rowp, 2 * own, ny)], (recv,), 1 << 21)
    recv = lax.all_to_all(back, "row", 0, 0, tiled=True)
    send, b, g0y, gly = call(
        functools.partial(y_send_kernel, nx),
        [(colp, 40, 128)] + [flat] * 3,
        (recv, bx, g0x, glx, u, my, py, faces),
        1 << 22,
        [flat, (nz, ny), (nz, ny), flat],
    )
    recv = lax.all_to_all(send, "col", 0, 0, tiled=True)
    (out,) = call(
        finish_kernel,
        [flat],
        (recv, b, g0y, gly, u, faces),
        1 << 22,
        [(colp + 1, 8, 128), flat, pltpu.SemaphoreType.DMA((8,))],
        out_specs=[HBM],
    )
    return out.reshape(nz, nx, ny)


def solution(mesh):
    in_specs = (P(None, "row", "col"), P(None, "row", "col"))
    out_specs = P(None, "row", "col")
    return jax.shard_map(
        on_device, mesh=mesh, in_specs=in_specs, out_specs=out_specs, check_vma=False
    )
```

```python
import functools

import jax
import jax.numpy as jnp
from jax import lax
from jax.experimental import pallas as pl
from jax.experimental.pallas import tpu as pltpu
from jax.sharding import PartitionSpec as P

z_weight = 0.02
F32 = jnp.float32
VMEM = pl.BlockSpec(memory_space=pltpu.VMEM)
HBM = pl.BlockSpec(memory_space=pltpu.HBM)


def call(kernel, outs, args, flops, scratch=(), specs=None, out_specs=None):
    return pl.pallas_call(
        kernel,
        out_shape=[jax.ShapeDtypeStruct(s, F32) for s in outs],
        in_specs=specs or [VMEM] * len(args),
        out_specs=out_specs or [VMEM] * len(outs),
        scratch_shapes=[pltpu.VMEM(s, F32) if isinstance(s, tuple) else s for s in scratch],
        compiler_params=pltpu.CompilerParams(vmem_limit_bytes=12 << 20),
        cost_estimate=pl.CostEstimate(flops=flops, bytes_accessed=1 << 20, transcendentals=0),
    )(*args)


def row(ref, j):
    start = j * 8 if isinstance(j, int) else pl.multiple_of(j * 8, 8)
    return ref[pl.ds(start, 8), :]


def put(ref, j, value):
    start = j * 8 if isinstance(j, int) else pl.multiple_of(j * 8, 8)
    ref[pl.ds(start, 8), :] = value


def tile(ref, nx, b, x):
    return ref[pl.ds(b * 8 * nx + x, 8, stride=nx), :]


def turn(tiles, target, b):
    target[pl.ds(b, 128, stride=8), :] = jnp.concatenate(tiles, axis=0).T


def turn_back(source, b):
    return source[pl.ds(b, 128, stride=8), :].T


def load_kernel(nx, u_hbm, k_hbm, u, k, ut, kt, low, high, sems):
    copies = [
        pltpu.make_async_copy(k_hbm, k, sems.at[0]),
        pltpu.make_async_copy(u_hbm, u, sems.at[1]),
    ]
    for copy in copies:
        copy.start()
    for copy, src, dst in zip(copies, (k, u), (kt, ut)):
        copy.wait()
        for b in range(8):
            turn([tile(src, nx, b, x) for x in range(nx)], dst, b)
    n = kt.shape[0] // 8
    low[0:8, :] = row(kt, 0)
    low[8:16, :] = row(ut, 0)
    high[0:8, :] = row(kt, n - 1)
    high[8:16, :] = row(ut, n - 1)


def pivots_kernel(nx, u, k, ut, kt, mx, px, r, ends, my, py, lt, rz):
    rows = u.shape[0]
    nz = rows // nx
    ny = lt.shape[0] // 8
    half = ny // 2

    def both(i, state):
        s, t, k_left, k_right = state
        j = ny - 1 - i
        next_left, next_right = row(kt, i + 1), row(kt, j - 1)
        e = 0.5 * (k_left + next_left)
        f = 0.5 * (k_right + next_right)
        inv_e = 1.0 / (s + e)
        inv_f = 1.0 / (t + f)
        m_left, m_right = e * inv_e, f * inv_f
        put(py, i, inv_e)
        put(py, j, inv_f)
        put(my, i, m_left)
        put(my, j, m_right)
        return 1.0 + s * m_left, 1.0 + t * m_right, next_left, next_right

    one = jnp.ones((8, 128), F32)
    s, t, k_left, k_right = lax.fori_loop(
        0, half - 1, both, (one, one, row(kt, 0), row(kt, ny - 1)), unroll=7
    )
    e = 0.5 * (k_left + k_right)
    inv = 1.0 / (s * t + e * (s + t))
    put(py, half - 1, (t + e) * inv)
    put(py, half, (s + e) * inv)
    put(my, half - 1, e * inv)
    put(my, half, e * inv)

    here_k, here_u = row(kt, 0), row(ut, 0)
    before = None
    for j in range(ny):
        if j + 1 < ny:
            next_k, next_u = row(kt, j + 1), row(ut, j + 1)
            flux = 0.5 * (here_k + next_k) * (next_u - here_u)
            put(lt, j, flux if before is None else flux - before)
            before, here_k, here_u = flux, next_k, next_u
        else:
            put(lt, j, -before)

    def at(ref, z):
        return ref[z * nx : (z + 1) * nx, :]

    uz, kz = at(u, 0), at(k, 0)
    below = (0.5 * z_weight) * kz * uz
    for z in range(nz):
        if z + 1 < nz:
            un, kn = at(u, z + 1), at(k, z + 1)
            above = (0.5 * z_weight) * (kz + kn) * (un - uz)
        else:
            un = kn = None
            above = -(0.5 * z_weight) * kz * uz
        rz[z * nx : (z + 1) * nx, :] = uz + (above - below)
        uz, kz, below = un, kn, above
    for b in range(8):
        side = turn_back(lt, b)
        for x in range(nx):
            start = (b * nx + x) * 8
            r[start : start + 8, :] = tile(rz, nx, b, x) + side[x * 8 : x * 8 + 8, :]

    def kx(i):
        return k[pl.ds(i, nz, stride=nx), :]

    mid = nx // 2
    s = t = jnp.ones((nz, 128), F32)
    k_left, k_right = kx(0), kx(nx - 1)
    ends[0] = k_left
    ends[1] = k_right
    for i in range(mid - 1):
        j = nx - 1 - i
        next_left, next_right = kx(i + 1), kx(j - 1)
        e = 0.5 * (k_left + next_left)
        f = 0.5 * (k_right + next_right)
        inv_e = 1.0 / (s + e)
        inv_f = 1.0 / (t + f)
        m_left, m_right = e * inv_e, f * inv_f
        px[i], px[j] = inv_e, inv_f
        mx[i], mx[j] = m_left, m_right
        s, t = 1.0 + s * m_left, 1.0 + t * m_right
        k_left, k_right = next_left, next_right
    e = 0.5 * (k_left + k_right)
    inv = 1.0 / (s * t + e * (s + t))
    px[mid - 1], px[mid] = (t + e) * inv, (s + e) * inv
    mx[mid - 1] = mx[mid] = e * inv


def x_send_kernel(nx, peers_y, low, high, from_left, from_right, r, ends, m, p, send, b, g0, gl, faces, turned):
    rows = r.shape[0]
    nz = rows // nx
    col = lax.axis_index("col")
    left = jnp.where(col == 0, 0.0, from_left[...])
    right = jnp.where(col == peers_y - 1, 0.0, from_right[...])
    k_low, u_low = low[0:8, :], low[8:16, :]
    k_high, u_high = high[0:8, :], high[8:16, :]
    face_left = 0.5 * (k_low + left[0:8, :])
    face_right = 0.5 * (k_high + right[0:8, :])
    faces[0:8, :] = jnp.sqrt(face_left)
    faces[8:16, :] = jnp.sqrt(face_right)
    turned[0:8, :] = face_left * (left[8:16, :] - u_low)
    turned[8:16, :] = face_right * (right[8:16, :] - u_high)
    turned[16:128, :] = jnp.zeros((112, 128), F32)
    corr = turned[...].T
    lane = lax.broadcasted_iota(jnp.int32, (128, 128), 1)
    peers = send.shape[0]
    own = nz // peers
    for t in range(8):
        zs = slice(t * 8, t * 8 + 8)
        west = jnp.where(lane == 0, corr[:, t : t + 1], 0.0)
        both = jnp.where(lane == 127, corr[:, 8 + t : 9 + t], west)

        def source(i):
            start = (t * nx + i) * 8
            return r[start : start + 8, :] + both[i * 8 : i * 8 + 8, :]

        mid = nx // 2
        ys, ws = {}, {}
        y, z = source(0), source(nx - 1)
        w = v = None
        for i in range(mid - 1):
            j = nx - 1 - i
            m_left, p_left = m[i, zs, :], p[i, zs, :]
            m_right, p_right = m[j, zs, :], p[j, zs, :]
            ys[i], ys[j] = y * p_left, z * p_right
            ws[i] = p_left if w is None else w * p_left
            ws[j] = p_right if v is None else v * p_right
            w = m_left if w is None else w * m_left
            v = m_right if v is None else v * m_right
            y = source(i + 1) + m_left * y
            z = source(j - 1) + m_right * z
        c_left, c_right, c_mid = p[mid - 1, zs, :], p[mid, zs, :], m[mid, zs, :]
        b_left, b_right = c_left * y + c_mid * z, c_right * z + c_mid * y
        g_left, g_right = c_left * w, c_mid * w
        h_left, h_right = c_mid * v, c_right * v
        for i in range(mid - 1, -1, -1):
            j = nx - 1 - i
            if i < mid - 1:
                m_left, m_right = m[i, zs, :], m[j, zs, :]
                b_left = ys[i] + m_left * b_left
                g_left = ws[i] + m_left * g_left
                h_left = m_left * h_left
                b_right = ys[j] + m_right * b_right
                g_right = m_right * g_right
                h_right = ws[j] + m_right * h_right
            b[i, zs, :], b[j, zs, :] = b_left, b_right
            g0[i, zs, :], g0[j, zs, :] = g_left, g_right
            gl[i, zs, :], gl[j, zs, :] = h_left, h_right
        parts = [g_left, g_right, h_right, b_left, b_right, ends[0, zs, :], ends[1, zs, :]]
        for q, part in enumerate(parts):
            for n in range(8 // own):
                d = t * (8 // own) + n
                send[d, q * own : (q + 1) * own, :] = part[n * own : (n + 1) * own, :]
    for d in range(peers):
        send[d, 7 * own : 8 * own, :] = jnp.zeros((own, 128), F32)


def solve(low, diag, up, rhs):
    n = len(diag)
    mid = n // 2
    c, q = [None] * n, [None] * n
    for order, near, far in (
        (range(mid), low, up),
        (range(n - 1, mid, -1), up, low),
    ):
        last = None
        for i in order:
            if last is None:
                inv = 1.0 / diag[i]
                q[i] = rhs[i] * inv
            else:
                inv = 1.0 / (diag[i] - near[i] * c[last])
                q[i] = (rhs[i] + near[i] * q[last]) * inv
            c[i] = far[i] * inv
            last = i
    i = mid
    inv = 1.0 / (diag[i] - low[i] * c[i - 1] - up[i] * c[i + 1])
    q[i] = (rhs[i] + low[i] * q[i - 1] + up[i] * q[i + 1]) * inv
    for i in range(mid - 1, -1, -1):
        q[i] = q[i] + c[i] * q[i + 1]
    for i in range(mid + 1, n):
        q[i] = q[i] + c[i] * q[i - 1]
    return q


def x_reduced_kernel(recv, send):
    peers = recv.shape[0]
    own = recv.shape[1] // 8
    nothing = (jnp.zeros((own, 128), F32),) * 7
    low, diag, up, rhs = [], [], [], []
    before = nothing
    for i in range(peers + 1):
        after = nothing
        if i < peers:
            after = tuple(recv[i, q * own : (q + 1) * own, :] for q in range(7))
        e = 0.5 * (before[6] + after[5])
        low.append(e * before[1])
        diag.append(1.0 + e * (before[2] + after[0]))
        up.append(e * after[1])
        rhs.append(e * (after[3] - before[4]))
        before = after
    flux = solve(low, diag, up, rhs)
    for d in range(peers):
        send[d, 0:own, :] = flux[d]
        send[d, own : 2 * own, :] = flux[d + 1]


def y_send_kernel(nx, recv, bx, g0x, glx, u, m, p, faces, send, b, g0, gl, dt, ql, qr):
    peers = recv.shape[0]
    own = recv.shape[1] // 2
    nz = peers * own
    ny = dt.shape[0] // 8
    half = ny // 2
    for d in range(peers):
        ql[d * own : (d + 1) * own, :] = recv[d, 0:own, :]
        qr[d * own : (d + 1) * own, :] = recv[d, own : 2 * own, :]
    for t in range(8):
        zs = slice(t * 8, t * 8 + 8)
        left, right = ql[zs, :], qr[zs, :]
        turn(
            [
                (bx[i, zs, :] - tile(u, nx, t, i))
                + (glx[i, zs, :] * right - g0x[i, zs, :] * left)
                for i in range(nx)
            ],
            dt,
            t,
        )

    w = x = jnp.ones((8, 128), F32)
    y, z = row(dt, 0), row(dt, ny - 1)
    for i in range(half - 1):
        j = ny - 1 - i
        m_left, p_left = row(m, i), row(p, i)
        m_right, p_right = row(m, j), row(p, j)
        put(b, i, y * p_left)
        put(g0, i, w * p_left)
        put(b, j, z * p_right)
        put(gl, j, x * p_right)
        y = row(dt, i + 1) + m_left * y
        w = w * m_left
        z = row(dt, j - 1) + m_right * z
        x = x * m_right
    c_left, c_right, c_mid = row(p, half - 1), row(p, half), row(m, half)
    b_left, b_right = c_left * y + c_mid * z, c_right * z + c_mid * y
    g_left, g_right = c_left * w, c_mid * w
    h_left, h_right = c_mid * x, c_right * x
    for i in range(half - 1, -1, -1):
        j = ny - 1 - i
        if i < half - 1:
            m_left, m_right = row(m, i), row(m, j)
            b_left = row(b, i) + m_left * b_left
            g_left = row(g0, i) + m_left * g_left
            h_left = m_left * h_left
            b_right = row(b, j) + m_right * b_right
            g_right = m_right * g_right
            h_right = row(gl, j) + m_right * h_right
        put(b, i, b_left)
        put(g0, i, g_left)
        put(gl, i, h_left)
        put(b, j, b_right)
        put(g0, j, g_right)
        put(gl, j, h_right)
    root_left, root_right = faces[0:8, :], faces[8:16, :]
    parts = [
        root_left * root_left * g_left,
        root_left * root_right * g_right,
        root_right * root_right * h_right,
        root_left * b_left,
        root_right * b_right,
    ]
    for d in range(send.shape[0]):
        for q, part in enumerate(parts):
            send[d, q * 8 : (q + 1) * 8, :] = part


def finish_kernel(nx, recv, b, g0, gl, u, faces, out, flux, whole, done, sems):
    peers = recv.shape[0]
    nothing = (jnp.zeros((8, 128), F32),) * 5
    low, diag, up, rhs = [], [], [], []
    before = nothing
    for i in range(peers + 1):
        after = nothing
        if i < peers:
            after = tuple(recv[i, q * 8 : (q + 1) * 8, :] for q in range(5))
        low.append(before[1])
        diag.append(1.0 + (before[2] + after[0]))
        up.append(after[1])
        rhs.append(after[3] - before[4])
        before = after
    q = solve(low, diag, up, rhs)
    for i in range(peers + 1):
        flux[i] = q[i]
    col = lax.axis_index("col")
    left = flux[col] * faces[0:8, :]
    right = flux[col + 1] * faces[8:16, :]
    for j in range(b.shape[0] // 8):
        put(whole, j, row(b, j) + (row(gl, j) * right - row(g0, j) * left))
    copies = []
    for i in range(8):
        delta = turn_back(whole, i)
        for x in range(nx):
            done[pl.ds(i * 128 + x, 8, stride=nx), :] = delta[x * 8 : x * 8 + 8, :]
        span = slice(i * 128, (i + 1) * 128)
        done[span, :] = u[span, :] + done[span, :]
        rows = pl.ds(i * 128, 128)
        copy = pltpu.make_async_copy(done.at[rows], out.at[rows], sems.at[i])
        copy.start()
        copies.append(copy)
    for copy in copies:
        copy.wait()


def on_device(field, conductivity):
    nz, nx, ny = field.shape
    rows = nz * nx
    rowp, colp = lax.axis_size("row"), lax.axis_size("col")
    own = nz // rowp
    u = field.reshape(rows, ny)
    k = conductivity.reshape(rows, ny)
    flat, cube = (rows, ny), (nx, nz, ny)
    uv, kv, ut, kt, low, high = call(
        functools.partial(load_kernel, nx),
        [flat] * 4 + [(16, 128)] * 2,
        tuple(pltpu.with_memory_space_constraint(a, pltpu.HBM) for a in (u, k)),
        1 << 20,
        [pltpu.SemaphoreType.DMA((2,))],
        [HBM, HBM],
    )
    up = [(i, (i + 1) % colp) for i in range(colp)]
    from_left = lax.ppermute(high, "col", up)
    from_right = lax.ppermute(low, "col", [(b, a) for a, b in up])
    mx, px, r, ends, my, py = call(
        functools.partial(pivots_kernel, nx),
        [cube] * 2 + [flat, (2, nz, ny)] + [flat] * 2,
        (uv, kv, ut, kt),
        1 << 23,
        [flat, flat],
    )
    send, bx, g0x, glx, faces = call(
        functools.partial(x_send_kernel, nx, colp),
        [(rowp, 8 * own, ny)] + [cube] * 3 + [(16, 128)],
        (low, high, from_left, from_right, r, ends, mx, px),
        1 << 22,
        [(128, 128)],
    )
    recv = lax.all_to_all(send, "row", 0, 0, tiled=True)
    (back,) = call(x_reduced_kernel, [(rowp, 2 * own, ny)], (recv,), 1 << 21)
    recv = lax.all_to_all(back, "row", 0, 0, tiled=True)
    send, b, g0y, gly = call(
        functools.partial(y_send_kernel, nx),
        [(colp, 40, 128)] + [flat] * 3,
        (recv, bx, g0x, glx, u, my, py, faces),
        1 << 22,
        [flat, (nz, ny), (nz, ny)],
    )
    recv = lax.all_to_all(send, "col", 0, 0, tiled=True)
    (out,) = call(
        functools.partial(finish_kernel, nx),
        [flat],
        (recv, b, g0y, gly, u, faces),
        1 << 22,
        [(colp + 1, 8, 128), flat, flat, pltpu.SemaphoreType.DMA((8,))],
        out_specs=[HBM],
    )
    return out.reshape(nz, nx, ny)


def solution(mesh):
    in_specs = (P(None, "row", "col"), P(None, "row", "col"))
    out_specs = P(None, "row", "col")
    return jax.shard_map(
        on_device, mesh=mesh, in_specs=in_specs, out_specs=out_specs, check_vma=False
    )
```

```python
import functools

import jax
import jax.numpy as jnp
from jax import lax
from jax.experimental import pallas as pl
from jax.experimental.pallas import tpu as pltpu
from jax.sharding import PartitionSpec as P

z_weight = 0.02
F32 = jnp.float32
VMEM = pl.BlockSpec(memory_space=pltpu.VMEM)
HBM = pl.BlockSpec(memory_space=pltpu.HBM)


def call(kernel, outs, args, flops, scratch=(), specs=None, out_specs=None):
    return pl.pallas_call(
        kernel,
        out_shape=[jax.ShapeDtypeStruct(s, F32) for s in outs],
        in_specs=specs or [VMEM] * len(args),
        out_specs=out_specs or [VMEM] * len(outs),
        scratch_shapes=[pltpu.VMEM(s, F32) if isinstance(s, tuple) else s for s in scratch],
        compiler_params=pltpu.CompilerParams(vmem_limit_bytes=12 << 20),
        cost_estimate=pl.CostEstimate(flops=flops, bytes_accessed=1 << 20, transcendentals=0),
    )(*args)


def row(ref, j):
    start = j * 8 if isinstance(j, int) else pl.multiple_of(j * 8, 8)
    return ref[pl.ds(start, 8), :]


def put(ref, j, value):
    start = j * 8 if isinstance(j, int) else pl.multiple_of(j * 8, 8)
    ref[pl.ds(start, 8), :] = value


def tile(ref, nx, b, x):
    return ref[pl.ds(b * 8 * nx + x, 8, stride=nx), :]


def turn(tiles, target, b):
    target[pl.ds(b, 128, stride=8), :] = jnp.concatenate(tiles, axis=0).T


def turn_back(source, b):
    return source[pl.ds(b, 128, stride=8), :].T


def load_kernel(nx, u_hbm, k_hbm, u, k, ut, kt, low, high, sems):
    copies = [
        pltpu.make_async_copy(k_hbm, k, sems.at[0]),
        pltpu.make_async_copy(u_hbm, u, sems.at[1]),
    ]
    for copy in copies:
        copy.start()
    for copy, src, dst in zip(copies, (k, u), (kt, ut)):
        copy.wait()
        for b in range(8):
            turn([tile(src, nx, b, x) for x in range(nx)], dst, b)
    n = kt.shape[0] // 8
    low[0:8, :] = row(kt, 0)
    low[8:16, :] = row(ut, 0)
    high[0:8, :] = row(kt, n - 1)
    high[8:16, :] = row(ut, n - 1)


def pivots_kernel(nx, u, k, ut, kt, mx, px, r, ends, my, py, lt, rz):
    rows = u.shape[0]
    nz = rows // nx
    ny = lt.shape[0] // 8
    half = ny // 2

    def both(i, state):
        s, t, k_left, k_right = state
        j = ny - 1 - i
        next_left, next_right = row(kt, i + 1), row(kt, j - 1)
        e = 0.5 * (k_left + next_left)
        f = 0.5 * (k_right + next_right)
        inv_e = 1.0 / (s + e)
        inv_f = 1.0 / (t + f)
        m_left, m_right = e * inv_e, f * inv_f
        put(py, i, inv_e)
        put(py, j, inv_f)
        put(my, i, m_left)
        put(my, j, m_right)
        return 1.0 + s * m_left, 1.0 + t * m_right, next_left, next_right

    one = jnp.ones((8, 128), F32)
    s, t, k_left, k_right = lax.fori_loop(
        0, half - 1, both, (one, one, row(kt, 0), row(kt, ny - 1)), unroll=7
    )
    e = 0.5 * (k_left + k_right)
    inv = 1.0 / (s * t + e * (s + t))
    put(py, half - 1, (t + e) * inv)
    put(py, half, (s + e) * inv)
    put(my, half - 1, e * inv)
    put(my, half, e * inv)

    here_k, here_u = row(kt, 0), row(ut, 0)
    before = None
    for j in range(ny):
        if j + 1 < ny:
            next_k, next_u = row(kt, j + 1), row(ut, j + 1)
            flux = 0.5 * (here_k + next_k) * (next_u - here_u)
            put(lt, j, flux if before is None else flux - before)
            before, here_k, here_u = flux, next_k, next_u
        else:
            put(lt, j, -before)

    def at(ref, z):
        return ref[z * nx : (z + 1) * nx, :]

    uz, kz = at(u, 0), at(k, 0)
    below = (0.5 * z_weight) * kz * uz
    for z in range(nz):
        if z + 1 < nz:
            un, kn = at(u, z + 1), at(k, z + 1)
            above = (0.5 * z_weight) * (kz + kn) * (un - uz)
        else:
            un = kn = None
            above = -(0.5 * z_weight) * kz * uz
        rz[z * nx : (z + 1) * nx, :] = uz + (above - below)
        uz, kz, below = un, kn, above
    for b in range(8):
        side = turn_back(lt, b)
        for x in range(nx):
            start = (b * nx + x) * 8
            r[start : start + 8, :] = tile(rz, nx, b, x) + side[x * 8 : x * 8 + 8, :]

    def kx(i):
        return k[pl.ds(i, nz, stride=nx), :]

    mid = nx // 2
    s = t = jnp.ones((nz, 128), F32)
    k_left, k_right = kx(0), kx(nx - 1)
    ends[0] = k_left
    ends[1] = k_right
    for i in range(mid - 1):
        j = nx - 1 - i
        next_left, next_right = kx(i + 1), kx(j - 1)
        e = 0.5 * (k_left + next_left)
        f = 0.5 * (k_right + next_right)
        inv_e = 1.0 / (s + e)
        inv_f = 1.0 / (t + f)
        m_left, m_right = e * inv_e, f * inv_f
        px[i], px[j] = inv_e, inv_f
        mx[i], mx[j] = m_left, m_right
        s, t = 1.0 + s * m_left, 1.0 + t * m_right
        k_left, k_right = next_left, next_right
    e = 0.5 * (k_left + k_right)
    inv = 1.0 / (s * t + e * (s + t))
    px[mid - 1], px[mid] = (t + e) * inv, (s + e) * inv
    mx[mid - 1] = mx[mid] = e * inv


def x_send_kernel(nx, peers_y, low, high, from_left, from_right, r, ends, m, p, send, b, g0, gl, faces, turned):
    rows = r.shape[0]
    nz = rows // nx
    col = lax.axis_index("col")
    left = jnp.where(col == 0, 0.0, from_left[...])
    right = jnp.where(col == peers_y - 1, 0.0, from_right[...])
    k_low, u_low = low[0:8, :], low[8:16, :]
    k_high, u_high = high[0:8, :], high[8:16, :]
    face_left = 0.5 * (k_low + left[0:8, :])
    face_right = 0.5 * (k_high + right[0:8, :])
    faces[0:8, :] = jnp.sqrt(face_left)
    faces[8:16, :] = jnp.sqrt(face_right)
    turned[0:8, :] = face_left * (left[8:16, :] - u_low)
    turned[8:16, :] = face_right * (right[8:16, :] - u_high)
    turned[16:128, :] = jnp.zeros((112, 128), F32)
    corr = turned[...].T
    lane = lax.broadcasted_iota(jnp.int32, (128, 128), 1)
    peers = send.shape[0]
    own = nz // peers
    for t in range(8):
        zs = slice(t * 8, t * 8 + 8)
        west = jnp.where(lane == 0, corr[:, t : t + 1], 0.0)
        both = jnp.where(lane == 127, corr[:, 8 + t : 9 + t], west)

        def source(i):
            start = (t * nx + i) * 8
            return r[start : start + 8, :] + both[i * 8 : i * 8 + 8, :]

        mid = nx // 2
        ys, ws = {}, {}
        y, z = source(0), source(nx - 1)
        w = v = None
        for i in range(mid - 1):
            j = nx - 1 - i
            m_left, p_left = m[i, zs, :], p[i, zs, :]
            m_right, p_right = m[j, zs, :], p[j, zs, :]
            ys[i], ys[j] = y * p_left, z * p_right
            ws[i] = p_left if w is None else w * p_left
            ws[j] = p_right if v is None else v * p_right
            w = m_left if w is None else w * m_left
            v = m_right if v is None else v * m_right
            y = source(i + 1) + m_left * y
            z = source(j - 1) + m_right * z
        c_left, c_right, c_mid = p[mid - 1, zs, :], p[mid, zs, :], m[mid, zs, :]
        b_left, b_right = c_left * y + c_mid * z, c_right * z + c_mid * y
        g_left, g_right = c_left * w, c_mid * w
        h_left, h_right = c_mid * v, c_right * v
        for i in range(mid - 1, -1, -1):
            j = nx - 1 - i
            if i < mid - 1:
                m_left, m_right = m[i, zs, :], m[j, zs, :]
                b_left = ys[i] + m_left * b_left
                g_left = ws[i] + m_left * g_left
                h_left = m_left * h_left
                b_right = ys[j] + m_right * b_right
                g_right = m_right * g_right
                h_right = ws[j] + m_right * h_right
            b[i, zs, :], b[j, zs, :] = b_left, b_right
            g0[i, zs, :], g0[j, zs, :] = g_left, g_right
            gl[i, zs, :], gl[j, zs, :] = h_left, h_right
        parts = [g_left, g_right, h_right, b_left, b_right, ends[0, zs, :], ends[1, zs, :]]
        for q, part in enumerate(parts):
            for n in range(8 // own):
                d = t * (8 // own) + n
                send[d, q * own : (q + 1) * own, :] = part[n * own : (n + 1) * own, :]
    for d in range(peers):
        send[d, 7 * own : 8 * own, :] = jnp.zeros((own, 128), F32)


def solve(low, diag, up, rhs):
    n = len(diag)
    mid = n // 2
    c, q = [None] * n, [None] * n
    for order, near, far in (
        (range(mid), low, up),
        (range(n - 1, mid, -1), up, low),
    ):
        last = None
        for i in order:
            if last is None:
                inv = 1.0 / diag[i]
                q[i] = rhs[i] * inv
            else:
                inv = 1.0 / (diag[i] - near[i] * c[last])
                q[i] = (rhs[i] + near[i] * q[last]) * inv
            c[i] = far[i] * inv
            last = i
    i = mid
    inv = 1.0 / (diag[i] - low[i] * c[i - 1] - up[i] * c[i + 1])
    q[i] = (rhs[i] + low[i] * q[i - 1] + up[i] * q[i + 1]) * inv
    for i in range(mid - 1, -1, -1):
        q[i] = q[i] + c[i] * q[i + 1]
    for i in range(mid + 1, n):
        q[i] = q[i] + c[i] * q[i - 1]
    return q


def x_reduced_kernel(recv, send):
    peers = recv.shape[0]
    own = recv.shape[1] // 8
    nothing = (jnp.zeros((own, 128), F32),) * 7
    low, diag, up, rhs = [], [], [], []
    before = nothing
    for i in range(peers + 1):
        after = nothing
        if i < peers:
            after = tuple(recv[i, q * own : (q + 1) * own, :] for q in range(7))
        e = 0.5 * (before[6] + after[5])
        low.append(e * before[1])
        diag.append(1.0 + e * (before[2] + after[0]))
        up.append(e * after[1])
        rhs.append(e * (after[3] - before[4]))
        before = after
    flux = solve(low, diag, up, rhs)
    for d in range(peers):
        send[d, 0:own, :] = flux[d]
        send[d, own : 2 * own, :] = flux[d + 1]


def y_send_kernel(nx, recv, bx, g0x, glx, u, m, p, faces, send, b, g0, gl, dt, ql, qr):
    peers = recv.shape[0]
    own = recv.shape[1] // 2
    nz = peers * own
    ny = dt.shape[0] // 8
    half = ny // 2
    for d in range(peers):
        ql[d * own : (d + 1) * own, :] = recv[d, 0:own, :]
        qr[d * own : (d + 1) * own, :] = recv[d, own : 2 * own, :]
    for t in range(8):
        zs = slice(t * 8, t * 8 + 8)
        left, right = ql[zs, :], qr[zs, :]
        turn(
            [
                (bx[i, zs, :] - tile(u, nx, t, i))
                + (glx[i, zs, :] * right - g0x[i, zs, :] * left)
                for i in range(nx)
            ],
            dt,
            t,
        )

    w = x = jnp.ones((8, 128), F32)
    y, z = row(dt, 0), row(dt, ny - 1)
    for i in range(half - 1):
        j = ny - 1 - i
        m_left, p_left = row(m, i), row(p, i)
        m_right, p_right = row(m, j), row(p, j)
        put(b, i, y * p_left)
        put(g0, i, w * p_left)
        put(b, j, z * p_right)
        put(gl, j, x * p_right)
        y = row(dt, i + 1) + m_left * y
        w = w * m_left
        z = row(dt, j - 1) + m_right * z
        x = x * m_right
    c_left, c_right, c_mid = row(p, half - 1), row(p, half), row(m, half)
    b_left, b_right = c_left * y + c_mid * z, c_right * z + c_mid * y
    g_left, g_right = c_left * w, c_mid * w
    h_left, h_right = c_mid * x, c_right * x
    for i in range(half - 1, -1, -1):
        j = ny - 1 - i
        if i < half - 1:
            m_left, m_right = row(m, i), row(m, j)
            b_left = row(b, i) + m_left * b_left
            g_left = row(g0, i) + m_left * g_left
            h_left = m_left * h_left
            b_right = row(b, j) + m_right * b_right
            g_right = m_right * g_right
            h_right = row(gl, j) + m_right * h_right
        put(b, i, b_left)
        put(g0, i, g_left)
        put(gl, i, h_left)
        put(b, j, b_right)
        put(g0, j, g_right)
        put(gl, j, h_right)
    root_left, root_right = faces[0:8, :], faces[8:16, :]
    parts = [
        root_left * root_left * g_left,
        root_left * root_right * g_right,
        root_right * root_right * h_right,
        root_left * b_left,
        root_right * b_right,
    ]
    for q, part in enumerate(parts):
        send[q * 8 : (q + 1) * 8, :] = part


def join_kernel(mine, other, both):
    both[0:40, :] = mine[...]
    both[40:80, :] = other[...]


def finish_kernel(nx, peers, *refs):
    got = refs[: peers // 2]
    b, g0, gl, u, faces, out, recv, flux, whole, done, sems = refs[peers // 2 :]
    col = lax.axis_index("col")
    for n, ref in zip([0] + [a // 2 for a in [4, 2, 6]], got):
        recv[lax.rem(col + peers - 2 * n, peers)] = ref[0:40, :]
        recv[lax.bitwise_xor(lax.rem(col + peers - 2 * n, peers), 1)] = ref[40:80, :]
    nothing = (jnp.zeros((8, 128), F32),) * 5
    low, diag, up, rhs = [], [], [], []
    before = nothing
    for i in range(peers + 1):
        after = nothing
        if i < peers:
            after = tuple(recv[i, q * 8 : (q + 1) * 8, :] for q in range(5))
        low.append(before[1])
        diag.append(1.0 + (before[2] + after[0]))
        up.append(after[1])
        rhs.append(after[3] - before[4])
        before = after
    q = solve(low, diag, up, rhs)
    for i in range(peers + 1):
        flux[i] = q[i]
    left = flux[col] * faces[0:8, :]
    right = flux[col + 1] * faces[8:16, :]
    for j in range(b.shape[0] // 8):
        put(whole, j, row(b, j) + (row(gl, j) * right - row(g0, j) * left))
    copies = []
    for i in range(8):
        delta = turn_back(whole, i)
        for x in range(nx):
            done[pl.ds(i * 128 + x, 8, stride=nx), :] = delta[x * 8 : x * 8 + 8, :]
        span = slice(i * 128, (i + 1) * 128)
        done[span, :] = u[span, :] + done[span, :]
        rows = pl.ds(i * 128, 128)
        copy = pltpu.make_async_copy(done.at[rows], out.at[rows], sems.at[i])
        copy.start()
        copies.append(copy)
    for copy in copies:
        copy.wait()


def on_device(field, conductivity):
    nz, nx, ny = field.shape
    rows = nz * nx
    rowp, colp = lax.axis_size("row"), lax.axis_size("col")
    own = nz // rowp
    u = field.reshape(rows, ny)
    k = conductivity.reshape(rows, ny)
    flat, cube = (rows, ny), (nx, nz, ny)
    uv, kv, ut, kt, low, high = call(
        functools.partial(load_kernel, nx),
        [flat] * 4 + [(16, 128)] * 2,
        tuple(pltpu.with_memory_space_constraint(a, pltpu.HBM) for a in (u, k)),
        1 << 20,
        [pltpu.SemaphoreType.DMA((2,))],
        [HBM, HBM],
    )
    up = [(i, (i + 1) % colp) for i in range(colp)]
    from_left = lax.ppermute(high, "col", up)
    from_right = lax.ppermute(low, "col", [(b, a) for a, b in up])
    mx, px, r, ends, my, py = call(
        functools.partial(pivots_kernel, nx),
        [cube] * 2 + [flat, (2, nz, ny)] + [flat] * 2,
        (uv, kv, ut, kt),
        1 << 23,
        [flat, flat],
    )
    send, bx, g0x, glx, faces = call(
        functools.partial(x_send_kernel, nx, colp),
        [(rowp, 8 * own, ny)] + [cube] * 3 + [(16, 128)],
        (low, high, from_left, from_right, r, ends, mx, px),
        1 << 22,
        [(128, 128)],
    )
    recv = lax.all_to_all(send, "row", 0, 0, tiled=True)
    (back,) = call(x_reduced_kernel, [(rowp, 2 * own, ny)], (recv,), 1 << 21)
    recv = lax.all_to_all(back, "row", 0, 0, tiled=True)
    send, b, g0y, gly = call(
        functools.partial(y_send_kernel, nx),
        [(40, 128)] + [flat] * 3,
        (recv, bx, g0x, glx, u, my, py, faces),
        1 << 22,
        [flat, (nz, ny), (nz, ny)],
    )
    other = lax.ppermute(send, "col", [(i, i ^ 1) for i in range(colp)])
    (both,) = call(join_kernel, [(80, 128)], (send, other), 1 << 16)
    got = [both]
    for step in [4, 2, 6]:
        got.append(lax.ppermute(both, "col", [(i, (i + step) % colp) for i in range(colp)]))
    (out,) = call(
        functools.partial(finish_kernel, nx, colp),
        [flat],
        (*got, b, g0y, gly, u, faces),
        1 << 22,
        [(colp, 40, 128), (colp + 1, 8, 128), flat, flat, pltpu.SemaphoreType.DMA((8,))],
        out_specs=[HBM],
    )
    return out.reshape(nz, nx, ny)


def solution(mesh):
    in_specs = (P(None, "row", "col"), P(None, "row", "col"))
    out_specs = P(None, "row", "col")
    return jax.shard_map(
        on_device, mesh=mesh, in_specs=in_specs, out_specs=out_specs, check_vma=False
    )
```

```python
import functools
import math

import jax
import jax.numpy as jnp
from jax import lax
from jax.experimental import pallas as pl
from jax.experimental.pallas import tpu as pltpu
from jax.sharding import PartitionSpec as P

z_weight = 0.02
F32 = jnp.float32
VMEM = pl.BlockSpec(memory_space=pltpu.VMEM)
HBM = pl.BlockSpec(memory_space=pltpu.HBM)


def call(kernel, outs, args, flops, scratch=(), specs=None, out_specs=None):
    return pl.pallas_call(
        kernel,
        out_shape=[jax.ShapeDtypeStruct(s, F32) for s in outs],
        in_specs=specs or [VMEM] * len(args),
        out_specs=out_specs or [VMEM] * len(outs),
        scratch_shapes=[pltpu.VMEM(s, F32) if isinstance(s, tuple) else s for s in scratch],
        compiler_params=pltpu.CompilerParams(vmem_limit_bytes=12 << 20),
        cost_estimate=pl.CostEstimate(flops=flops, bytes_accessed=1 << 20, transcendentals=0),
    )(*args)


def row(ref, j):
    start = j * 8 if isinstance(j, int) else pl.multiple_of(j * 8, 8)
    return ref[pl.ds(start, 8), :]


def put(ref, j, value):
    start = j * 8 if isinstance(j, int) else pl.multiple_of(j * 8, 8)
    ref[pl.ds(start, 8), :] = value


def tile(ref, nx, b, x):
    return ref[pl.ds(b * 8 * nx + x, 8, stride=nx), :]


def turn(tiles, target, b):
    target[pl.ds(b, 128, stride=8), :] = jnp.concatenate(tiles, axis=0).T


def turn_back(source, b):
    return source[pl.ds(b, 128, stride=8), :].T


def load_kernel(nx, u_hbm, k_hbm, u, k, ut, kt, low, high, sems):
    copies = [
        pltpu.make_async_copy(k_hbm, k, sems.at[0]),
        pltpu.make_async_copy(u_hbm, u, sems.at[1]),
    ]
    for copy in copies:
        copy.start()
    for copy, src, dst in zip(copies, (k, u), (kt, ut)):
        copy.wait()
        for b in range(8):
            turn([tile(src, nx, b, x) for x in range(nx)], dst, b)
    n = kt.shape[0] // 8
    low[0:8, :] = row(kt, 0)
    low[8:16, :] = row(ut, 0)
    high[0:8, :] = row(kt, n - 1)
    high[8:16, :] = row(ut, n - 1)


def pivots_kernel(nx, u, k, ut, kt, mx, px, r, ends, my, py, lt, rz):
    rows = u.shape[0]
    nz = rows // nx
    ny = lt.shape[0] // 8
    half = ny // 2

    def both(i, state):
        s, t, k_left, k_right = state
        j = ny - 1 - i
        next_left, next_right = row(kt, i + 1), row(kt, j - 1)
        e = 0.5 * (k_left + next_left)
        f = 0.5 * (k_right + next_right)
        inv_e = 1.0 / (s + e)
        inv_f = 1.0 / (t + f)
        m_left, m_right = e * inv_e, f * inv_f
        put(py, i, inv_e)
        put(py, j, inv_f)
        put(my, i, m_left)
        put(my, j, m_right)
        return 1.0 + s * m_left, 1.0 + t * m_right, next_left, next_right

    one = jnp.ones((8, 128), F32)
    s, t, k_left, k_right = lax.fori_loop(
        0, half - 1, both, (one, one, row(kt, 0), row(kt, ny - 1)), unroll=7
    )
    e = 0.5 * (k_left + k_right)
    inv = 1.0 / (s * t + e * (s + t))
    put(py, half - 1, (t + e) * inv)
    put(py, half, (s + e) * inv)
    put(my, half - 1, e * inv)
    put(my, half, e * inv)

    here_k, here_u = row(kt, 0), row(ut, 0)
    before = None
    for j in range(ny):
        if j + 1 < ny:
            next_k, next_u = row(kt, j + 1), row(ut, j + 1)
            flux = 0.5 * (here_k + next_k) * (next_u - here_u)
            put(lt, j, flux if before is None else flux - before)
            before, here_k, here_u = flux, next_k, next_u
        else:
            put(lt, j, -before)

    def at(ref, z):
        return ref[z * nx : (z + 1) * nx, :]

    uz, kz = at(u, 0), at(k, 0)
    below = (0.5 * z_weight) * kz * uz
    for z in range(nz):
        if z + 1 < nz:
            un, kn = at(u, z + 1), at(k, z + 1)
            above = (0.5 * z_weight) * (kz + kn) * (un - uz)
        else:
            un = kn = None
            above = -(0.5 * z_weight) * kz * uz
        rz[z * nx : (z + 1) * nx, :] = uz + (above - below)
        uz, kz, below = un, kn, above
    for b in range(8):
        side = turn_back(lt, b)
        for x in range(nx):
            start = (b * nx + x) * 8
            r[start : start + 8, :] = tile(rz, nx, b, x) + side[x * 8 : x * 8 + 8, :]

    def kx(i):
        return k[pl.ds(i, nz, stride=nx), :]

    mid = nx // 2
    s = t = jnp.ones((nz, 128), F32)
    k_left, k_right = kx(0), kx(nx - 1)
    ends[0] = k_left
    ends[1] = k_right
    for i in range(mid - 1):
        j = nx - 1 - i
        next_left, next_right = kx(i + 1), kx(j - 1)
        e = 0.5 * (k_left + next_left)
        f = 0.5 * (k_right + next_right)
        inv_e = 1.0 / (s + e)
        inv_f = 1.0 / (t + f)
        m_left, m_right = e * inv_e, f * inv_f
        px[i], px[j] = inv_e, inv_f
        mx[i], mx[j] = m_left, m_right
        s, t = 1.0 + s * m_left, 1.0 + t * m_right
        k_left, k_right = next_left, next_right
    e = 0.5 * (k_left + k_right)
    inv = 1.0 / (s * t + e * (s + t))
    px[mid - 1], px[mid] = (t + e) * inv, (s + e) * inv
    mx[mid - 1] = mx[mid] = e * inv


def x_send_kernel(nx, peers_y, group, low, high, from_left, from_right, r, ends, m, p, *refs):
    sends = refs[:group]
    b, g0, gl, faces, turned, send = refs[group:]
    rows = r.shape[0]
    nz = rows // nx
    col = lax.axis_index("col")
    left = jnp.where(col == 0, 0.0, from_left[...])
    right = jnp.where(col == peers_y - 1, 0.0, from_right[...])
    k_low, u_low = low[0:8, :], low[8:16, :]
    k_high, u_high = high[0:8, :], high[8:16, :]
    face_left = 0.5 * (k_low + left[0:8, :])
    face_right = 0.5 * (k_high + right[0:8, :])
    faces[0:8, :] = jnp.sqrt(face_left)
    faces[8:16, :] = jnp.sqrt(face_right)
    turned[0:8, :] = face_left * (left[8:16, :] - u_low)
    turned[8:16, :] = face_right * (right[8:16, :] - u_high)
    turned[16:128, :] = jnp.zeros((112, 128), F32)
    corr = turned[...].T
    lane = lax.broadcasted_iota(jnp.int32, (128, 128), 1)
    own = nz // group
    for t in range(8):
        zs = slice(t * 8, t * 8 + 8)
        west = jnp.where(lane == 0, corr[:, t : t + 1], 0.0)
        both = jnp.where(lane == 127, corr[:, 8 + t : 9 + t], west)

        def source(i):
            start = (t * nx + i) * 8
            return r[start : start + 8, :] + both[i * 8 : i * 8 + 8, :]

        mid = nx // 2
        ys, ws = {}, {}
        y, z = source(0), source(nx - 1)
        w = v = None
        for i in range(mid - 1):
            j = nx - 1 - i
            m_left, p_left = m[i, zs, :], p[i, zs, :]
            m_right, p_right = m[j, zs, :], p[j, zs, :]
            ys[i], ys[j] = y * p_left, z * p_right
            ws[i] = p_left if w is None else w * p_left
            ws[j] = p_right if v is None else v * p_right
            w = m_left if w is None else w * m_left
            v = m_right if v is None else v * m_right
            y = source(i + 1) + m_left * y
            z = source(j - 1) + m_right * z
        c_left, c_right, c_mid = p[mid - 1, zs, :], p[mid, zs, :], m[mid, zs, :]
        b_left, b_right = c_left * y + c_mid * z, c_right * z + c_mid * y
        g_left, g_right = c_left * w, c_mid * w
        h_left, h_right = c_mid * v, c_right * v
        for i in range(mid - 1, -1, -1):
            j = nx - 1 - i
            if i < mid - 1:
                m_left, m_right = m[i, zs, :], m[j, zs, :]
                b_left = ys[i] + m_left * b_left
                g_left = ws[i] + m_left * g_left
                h_left = m_left * h_left
                b_right = ys[j] + m_right * b_right
                g_right = m_right * g_right
                h_right = ws[j] + m_right * h_right
            b[i, zs, :], b[j, zs, :] = b_left, b_right
            g0[i, zs, :], g0[j, zs, :] = g_left, g_right
            gl[i, zs, :], gl[j, zs, :] = h_left, h_right
        parts = [g_left, g_right, h_right, b_left, b_right, ends[0, zs, :], ends[1, zs, :]]
        for q, part in enumerate(parts):
            start = q * own + t * 8 % own
            send[t * 8 // own, start : start + 8, :] = part
    mine = lax.rem(lax.axis_index("row"), group)
    for step, out in enumerate(sends):
        out[...] = send[lax.rem(mine + step, group)]


def solve(low, diag, up, rhs):
    n = len(diag)
    mid = n // 2
    c, q = [None] * n, [None] * n
    for order, near, far in (
        (range(mid), low, up),
        (range(n - 1, mid, -1), up, low),
    ):
        last = None
        for i in order:
            if last is None:
                inv = 1.0 / diag[i]
                q[i] = rhs[i] * inv
            else:
                inv = 1.0 / (diag[i] - near[i] * c[last])
                q[i] = (rhs[i] + near[i] * q[last]) * inv
            c[i] = far[i] * inv
            last = i
    i = mid
    inv = 1.0 / (diag[i] - low[i] * c[i - 1] - up[i] * c[i + 1])
    q[i] = (rhs[i] + low[i] * q[i - 1] + up[i] * q[i + 1]) * inv
    for i in range(mid - 1, -1, -1):
        q[i] = q[i] + c[i] * q[i + 1]
    for i in range(mid + 1, n):
        q[i] = q[i] + c[i] * q[i - 1]
    return q


def system(blocks, nothing):
    low, diag, up, rhs = [], [], [], []
    for before, after in zip([nothing] + blocks, blocks + [nothing]):
        e = 0.5 * (before[6] + after[5])
        low.append(e * before[1])
        diag.append(1.0 + e * (before[2] + after[0]))
        up.append(e * after[1])
        rhs.append(e * (after[3] - before[4]))
    return low, diag, up, rhs


def merge_kernel(group, *refs):
    got, sup, inner, recv = refs[:group], refs[group], refs[group + 1], refs[group + 2]
    own = sup.shape[0] // 7
    mine = lax.rem(lax.axis_index("row"), group)
    for step, ref in enumerate(got):
        recv[lax.rem(mine + group - step, group)] = ref[...]
    blocks = [tuple(recv[d, q * own : (q + 1) * own, :] for q in range(7)) for d in range(group)]
    low, diag, up, rhs = system(blocks, blocks[0])
    low, diag, up, rhs = low[1:group], diag[1:group], up[1:group], rhs[1:group]
    inv = 1.0 / diag[0]
    c_first, a_first, b_first = up[0] * inv, rhs[0] * inv, low[0] * inv
    inv = 1.0 / diag[2]
    c_last, a_last, g_last = low[2] * inv, rhs[2] * inv, up[2] * inv
    inv = 1.0 / (diag[1] - low[1] * c_first - up[1] * c_last)
    a_mid = (rhs[1] + low[1] * a_first + up[1] * a_last) * inv
    b_mid = low[1] * b_first * inv
    g_mid = up[1] * g_last * inv
    a_first, b_first, g_first = a_first + c_first * a_mid, b_first + c_first * b_mid, c_first * g_mid
    a_last, b_last, g_last = a_last + c_last * a_mid, c_last * b_mid, g_last + c_last * g_mid
    first, last = blocks[0], blocks[group - 1]
    parts = [
        first[0] - first[1] * b_first,
        first[1] * g_first,
        last[2] - last[1] * g_last,
        first[3] + first[1] * a_first,
        last[4] - last[1] * a_last,
        first[5],
        last[6],
    ]
    for q, part in enumerate(parts):
        sup[q * own : (q + 1) * own, :] = part
    kept = [a_first, a_mid, a_last, b_first, b_mid, b_last, g_first, g_mid, g_last]
    for q, part in enumerate(kept):
        inner[q * own : (q + 1) * own, :] = part


def flux_kernel(group, *refs):
    got, inner, sends = refs[:group], refs[group], refs[group + 1 : 2 * group + 1]
    recv, flux, send = refs[2 * group + 1 :]
    own = got[0].shape[0] // 7
    row_index = lax.axis_index("row")
    mine, outer = lax.rem(row_index, group), lax.div(row_index, group)
    for step, ref in enumerate(got):
        recv[lax.rem(outer + group - step, group)] = ref[...]
    blocks = [tuple(recv[d, q * own : (q + 1) * own, :] for q in range(7)) for d in range(group)]
    q = solve(*system(blocks, (jnp.zeros((own, 128), F32),) * 7))
    for i in range(group + 1):
        flux[i] = q[i]
    left, right = flux[outer], flux[outer + 1]

    def kept(i):
        return inner[i * own : (i + 1) * own, :]

    q = [left]
    for i in range(group - 1):
        q.append(kept(i) + kept(group - 1 + i) * left + kept(2 * group - 2 + i) * right)
    q.append(right)
    for d in range(group):
        send[d, 0:own, :] = q[d]
        send[d, own : 2 * own, :] = q[d + 1]
    for step, out in enumerate(sends):
        out[...] = send[lax.rem(mine + step, group)]


def y_send_kernel(nx, group, *refs):
    got = refs[:group]
    bx, g0x, glx, u, m, p, faces, send, b, g0, gl, dt, ql, qr = refs[group:]
    own = got[0].shape[0] // 2
    ny = dt.shape[0] // 8
    half = ny // 2
    mine = lax.rem(lax.axis_index("row"), group)
    for step, ref in enumerate(got):
        start = pl.multiple_of(lax.rem(mine + group - step, group) * own, own)
        ql[pl.ds(start, own), :] = ref[0:own, :]
        qr[pl.ds(start, own), :] = ref[own : 2 * own, :]
    for t in range(8):
        zs = slice(t * 8, t * 8 + 8)
        left, right = ql[zs, :], qr[zs, :]
        turn(
            [
                (bx[i, zs, :] - tile(u, nx, t, i))
                + (glx[i, zs, :] * right - g0x[i, zs, :] * left)
                for i in range(nx)
            ],
            dt,
            t,
        )

    w = x = jnp.ones((8, 128), F32)
    y, z = row(dt, 0), row(dt, ny - 1)
    for i in range(half - 1):
        j = ny - 1 - i
        m_left, p_left = row(m, i), row(p, i)
        m_right, p_right = row(m, j), row(p, j)
        put(b, i, y * p_left)
        put(g0, i, w * p_left)
        put(b, j, z * p_right)
        put(gl, j, x * p_right)
        y = row(dt, i + 1) + m_left * y
        w = w * m_left
        z = row(dt, j - 1) + m_right * z
        x = x * m_right
    c_left, c_right, c_mid = row(p, half - 1), row(p, half), row(m, half)
    b_left, b_right = c_left * y + c_mid * z, c_right * z + c_mid * y
    g_left, g_right = c_left * w, c_mid * w
    h_left, h_right = c_mid * x, c_right * x
    for i in range(half - 1, -1, -1):
        j = ny - 1 - i
        if i < half - 1:
            m_left, m_right = row(m, i), row(m, j)
            b_left = row(b, i) + m_left * b_left
            g_left = row(g0, i) + m_left * g_left
            h_left = m_left * h_left
            b_right = row(b, j) + m_right * b_right
            g_right = m_right * g_right
            h_right = row(gl, j) + m_right * h_right
        put(b, i, b_left)
        put(g0, i, g_left)
        put(gl, i, h_left)
        put(b, j, b_right)
        put(g0, j, g_right)
        put(gl, j, h_right)
    root_left, root_right = faces[0:8, :], faces[8:16, :]
    parts = [
        root_left * root_left * g_left,
        root_left * root_right * g_right,
        root_right * root_right * h_right,
        root_left * b_left,
        root_right * b_right,
    ]
    for q, part in enumerate(parts):
        send[q * 8 : (q + 1) * 8, :] = part


def join_kernel(mine, other, both):
    both[0:40, :] = mine[...]
    both[40:80, :] = other[...]


def finish_kernel(nx, peers, *refs):
    got = refs[: peers // 2]
    b, g0, gl, u, faces, out, recv, flux, whole, done, sems = refs[peers // 2 :]
    col = lax.axis_index("col")
    for n, ref in zip([0] + [a // 2 for a in [4, 2, 6]], got):
        recv[lax.rem(col + peers - 2 * n, peers)] = ref[0:40, :]
        recv[lax.bitwise_xor(lax.rem(col + peers - 2 * n, peers), 1)] = ref[40:80, :]
    nothing = (jnp.zeros((8, 128), F32),) * 5
    low, diag, up, rhs = [], [], [], []
    before = nothing
    for i in range(peers + 1):
        after = nothing
        if i < peers:
            after = tuple(recv[i, q * 8 : (q + 1) * 8, :] for q in range(5))
        low.append(before[1])
        diag.append(1.0 + (before[2] + after[0]))
        up.append(after[1])
        rhs.append(after[3] - before[4])
        before = after
    q = solve(low, diag, up, rhs)
    for i in range(peers + 1):
        flux[i] = q[i]
    left = flux[col] * faces[0:8, :]
    right = flux[col + 1] * faces[8:16, :]
    for j in range(b.shape[0] // 8):
        put(whole, j, row(b, j) + (row(gl, j) * right - row(g0, j) * left))
    copies = []
    for i in range(8):
        delta = turn_back(whole, i)
        for x in range(nx):
            done[pl.ds(i * 128 + x, 8, stride=nx), :] = delta[x * 8 : x * 8 + 8, :]
        span = slice(i * 128, (i + 1) * 128)
        done[span, :] = u[span, :] + done[span, :]
        rows = pl.ds(i * 128, 128)
        copy = pltpu.make_async_copy(done.at[rows], out.at[rows], sems.at[i])
        copy.start()
        copies.append(copy)
    for copy in copies:
        copy.wait()


def on_device(field, conductivity):
    nz, nx, ny = field.shape
    rows = nz * nx
    rowp, colp = lax.axis_size("row"), lax.axis_size("col")
    u = field.reshape(rows, ny)
    k = conductivity.reshape(rows, ny)
    flat, cube = (rows, ny), (nx, nz, ny)
    uv, kv, ut, kt, low, high = call(
        functools.partial(load_kernel, nx),
        [flat] * 4 + [(16, 128)] * 2,
        tuple(pltpu.with_memory_space_constraint(a, pltpu.HBM) for a in (u, k)),
        1 << 20,
        [pltpu.SemaphoreType.DMA((2,))],
        [HBM, HBM],
    )
    up = [(i, (i + 1) % colp) for i in range(colp)]
    from_left = lax.ppermute(high, "col", up)
    from_right = lax.ppermute(low, "col", [(b, a) for a, b in up])
    mx, px, r, ends, my, py = call(
        functools.partial(pivots_kernel, nx),
        [cube] * 2 + [flat, (2, nz, ny)] + [flat] * 2,
        (uv, kv, ut, kt),
        1 << 23,
        [flat, flat],
    )
    group = math.isqrt(rowp)
    own = nz // group
    inside, across = {}, {}
    for step in range(group):
        inside[step] = [(i, i // group * group + (i + step) % group) for i in range(rowp)]
        across[step] = [(i, (i + step * group) % rowp) for i in range(rowp)]
    order = sorted(range(1, group), key=lambda step: abs(step - group // 2))

    def exchange(arrays, pairs):
        got = list(arrays)
        for step in order:
            got[step] = lax.ppermute(arrays[step], "row", pairs[step])
        return got

    *parts, bx, g0x, glx, faces = call(
        functools.partial(x_send_kernel, nx, colp, group),
        [(7 * own, ny)] * group + [cube] * 3 + [(16, 128)],
        (low, high, from_left, from_right, r, ends, mx, px),
        1 << 22,
        [(128, 128), (group, 7 * own, ny)],
    )
    parts = exchange(parts, inside)
    merged, inner = call(
        functools.partial(merge_kernel, group),
        [(7 * own, ny), (9 * own, ny)],
        parts,
        1 << 20,
        [(group, 7 * own, ny)],
    )
    parts = exchange([merged] * group, across)
    parts = call(
        functools.partial(flux_kernel, group),
        [(2 * own, ny)] * group,
        (*parts, inner),
        1 << 20,
        [(group, 7 * own, ny), (group + 1, own, ny), (group, 2 * own, ny)],
    )
    parts = exchange(parts, inside)
    send, b, g0y, gly = call(
        functools.partial(y_send_kernel, nx, group),
        [(40, 128)] + [flat] * 3,
        (*parts, bx, g0x, glx, u, my, py, faces),
        1 << 22,
        [flat, (nz, ny), (nz, ny)],
    )
    other = lax.ppermute(send, "col", [(i, i ^ 1) for i in range(colp)])
    (both,) = call(join_kernel, [(80, 128)], (send, other), 1 << 16)
    got = [both]
    for step in [4, 2, 6]:
        got.append(lax.ppermute(both, "col", [(i, (i + step) % colp) for i in range(colp)]))
    (out,) = call(
        functools.partial(finish_kernel, nx, colp),
        [flat],
        (*got, b, g0y, gly, u, faces),
        1 << 22,
        [(colp, 40, 128), (colp + 1, 8, 128), flat, flat, pltpu.SemaphoreType.DMA((8,))],
        out_specs=[HBM],
    )
    return out.reshape(nz, nx, ny)


def solution(mesh):
    in_specs = (P(None, "row", "col"), P(None, "row", "col"))
    out_specs = P(None, "row", "col")
    return jax.shard_map(
        on_device, mesh=mesh, in_specs=in_specs, out_specs=out_specs, check_vma=False
    )
```

```python
import functools
import math

import jax
import jax.numpy as jnp
from jax import lax
from jax.experimental import pallas as pl
from jax.experimental.pallas import tpu as pltpu
from jax.sharding import PartitionSpec as P

z_weight = 0.02
F32 = jnp.float32
VMEM = pl.BlockSpec(memory_space=pltpu.VMEM)
HBM = pl.BlockSpec(memory_space=pltpu.HBM)


def call(kernel, outs, args, flops, scratch=(), specs=None, out_specs=None):
    return pl.pallas_call(
        kernel,
        out_shape=[jax.ShapeDtypeStruct(s, F32) for s in outs],
        in_specs=specs or [VMEM] * len(args),
        out_specs=out_specs or [VMEM] * len(outs),
        scratch_shapes=[pltpu.VMEM(s, F32) if isinstance(s, tuple) else s for s in scratch],
        compiler_params=pltpu.CompilerParams(vmem_limit_bytes=12 << 20),
        cost_estimate=pl.CostEstimate(flops=flops, bytes_accessed=1 << 20, transcendentals=0),
    )(*args)


def row(ref, j):
    start = j * 8 if isinstance(j, int) else pl.multiple_of(j * 8, 8)
    return ref[pl.ds(start, 8), :]


def put(ref, j, value):
    start = j * 8 if isinstance(j, int) else pl.multiple_of(j * 8, 8)
    ref[pl.ds(start, 8), :] = value


def tile(ref, nx, b, x):
    return ref[pl.ds(b * 8 * nx + x, 8, stride=nx), :]


def turn(tiles, target, b):
    target[pl.ds(b, 128, stride=8), :] = jnp.concatenate(tiles, axis=0).T


def turn_back(source, b):
    return source[pl.ds(b, 128, stride=8), :].T


def load_kernel(nx, u_hbm, k_hbm, u, k, ut, kt, low, high, sems):
    copies = [
        pltpu.make_async_copy(k_hbm, k, sems.at[0]),
        pltpu.make_async_copy(u_hbm, u, sems.at[1]),
    ]
    for copy in copies:
        copy.start()
    for copy, src, dst in zip(copies, (k, u), (kt, ut)):
        copy.wait()
        for b in range(8):
            turn([tile(src, nx, b, x) for x in range(nx)], dst, b)
    n = kt.shape[0] // 8
    low[0:8, :] = row(kt, 0)
    low[8:16, :] = row(ut, 0)
    high[0:8, :] = row(kt, n - 1)
    high[8:16, :] = row(ut, n - 1)


def pivots_kernel(nx, u, k, ut, kt, mx, px, g0, gl, r, ends, lt, rz):
    rows = u.shape[0]
    nz = rows // nx
    ny = lt.shape[0] // 8

    here_k, here_u = row(kt, 0), row(ut, 0)
    before = None
    for j in range(ny):
        if j + 1 < ny:
            next_k, next_u = row(kt, j + 1), row(ut, j + 1)
            flux = 0.5 * (here_k + next_k) * (next_u - here_u)
            put(lt, j, flux if before is None else flux - before)
            before, here_k, here_u = flux, next_k, next_u
        else:
            put(lt, j, -before)

    def at(ref, z):
        return ref[z * nx : (z + 1) * nx, :]

    uz, kz = at(u, 0), at(k, 0)
    below = (0.5 * z_weight) * kz * uz
    for z in range(nz):
        if z + 1 < nz:
            un, kn = at(u, z + 1), at(k, z + 1)
            above = (0.5 * z_weight) * (kz + kn) * (un - uz)
        else:
            un = kn = None
            above = -(0.5 * z_weight) * kz * uz
        rz[z * nx : (z + 1) * nx, :] = uz + (above - below)
        uz, kz, below = un, kn, above
    for b in range(8):
        side = turn_back(lt, b)
        for x in range(nx):
            start = (b * nx + x) * 8
            r[start : start + 8, :] = tile(rz, nx, b, x) + side[x * 8 : x * 8 + 8, :]

    def kx(i):
        return k[pl.ds(i, nz, stride=nx), :]

    mid = nx // 2
    s = t = jnp.ones((nz, 128), F32)
    k_left, k_right = kx(0), kx(nx - 1)
    ends[0] = k_left
    ends[1] = k_right
    for i in range(mid - 1):
        j = nx - 1 - i
        next_left, next_right = kx(i + 1), kx(j - 1)
        e = 0.5 * (k_left + next_left)
        f = 0.5 * (k_right + next_right)
        inv_e = 1.0 / (s + e)
        inv_f = 1.0 / (t + f)
        m_left, m_right = e * inv_e, f * inv_f
        px[i], px[j] = inv_e, inv_f
        mx[i], mx[j] = m_left, m_right
        s, t = 1.0 + s * m_left, 1.0 + t * m_right
        k_left, k_right = next_left, next_right
    e = 0.5 * (k_left + k_right)
    inv = 1.0 / (s * t + e * (s + t))
    c_left, c_right, c_mid = (t + e) * inv, (s + e) * inv, e * inv
    px[mid - 1], px[mid] = c_left, c_right
    mx[mid - 1] = mx[mid] = c_mid
    w = v = jnp.ones((nz, 128), F32)
    for i in range(mid - 1):
        j = nx - 1 - i
        g0[i], gl[j] = w * px[i], v * px[j]
        w, v = w * mx[i], v * mx[j]
    g_left, g_right = c_left * w, c_mid * w
    h_left, h_right = c_mid * v, c_right * v
    for i in range(mid - 1, -1, -1):
        j = nx - 1 - i
        if i < mid - 1:
            m_left, m_right = mx[i], mx[j]
            g_left, h_left = g0[i] + m_left * g_left, m_left * h_left
            g_right, h_right = m_right * g_right, gl[j] + m_right * h_right
        g0[i], g0[j] = g_left, g_right
        gl[i], gl[j] = h_left, h_right


def x_send_kernel(nx, peers_y, group, low, high, from_left, from_right, r, ends, g0, gl, *refs):
    sends = refs[:group]
    full, faces, turned, send = refs[group:]
    rows = r.shape[0]
    nz = rows // nx
    col = lax.axis_index("col")
    left = jnp.where(col == 0, 0.0, from_left[...])
    right = jnp.where(col == peers_y - 1, 0.0, from_right[...])
    k_low, u_low = low[0:8, :], low[8:16, :]
    k_high, u_high = high[0:8, :], high[8:16, :]
    face_left = 0.5 * (k_low + left[0:8, :])
    face_right = 0.5 * (k_high + right[0:8, :])
    faces[0:8, :] = jnp.sqrt(face_left)
    faces[8:16, :] = jnp.sqrt(face_right)
    turned[0:8, :] = face_left * (left[8:16, :] - u_low)
    turned[8:16, :] = face_right * (right[8:16, :] - u_high)
    turned[16:128, :] = jnp.zeros((112, 128), F32)
    corr = turned[...].T
    lane = lax.broadcasted_iota(jnp.int32, (128, 128), 1)
    own = nz // group
    for t in range(8):
        zs = slice(t * 8, t * 8 + 8)
        west = jnp.where(lane == 0, corr[:, t : t + 1], 0.0)
        both = jnp.where(lane == 127, corr[:, 8 + t : 9 + t], west)

        zero = jnp.zeros((8, 128), F32)
        b0, bl = [zero, zero], [zero, zero]
        for i in range(nx):
            start = (t * nx + i) * 8
            ri = r[start : start + 8, :] + both[i * 8 : i * 8 + 8, :]
            full[start : start + 8, :] = ri
            b0[i % 2] = b0[i % 2] + g0[i, zs, :] * ri
            bl[i % 2] = bl[i % 2] + gl[i, zs, :] * ri
        parts = [
            g0[0, zs, :],
            g0[nx - 1, zs, :],
            gl[nx - 1, zs, :],
            b0[0] + b0[1],
            bl[0] + bl[1],
            ends[0, zs, :],
            ends[1, zs, :],
        ]
        for q, part in enumerate(parts):
            start = q * own + t * 8 % own
            send[t * 8 // own, start : start + 8, :] = part
    mine = lax.rem(lax.axis_index("row"), group)
    for step, out in enumerate(sends):
        out[...] = send[lax.rem(mine + step, group)]


def x_inner_kernel(nx, r, m, p, b):
    mid = nx // 2
    for t in range(8):
        zs = slice(t * 8, t * 8 + 8)

        def source(i):
            start = (t * nx + i) * 8
            return r[start : start + 8, :]

        ys = {}
        y, z = source(0), source(nx - 1)
        for i in range(mid - 1):
            j = nx - 1 - i
            ys[i], ys[j] = y * p[i, zs, :], z * p[j, zs, :]
            y = source(i + 1) + m[i, zs, :] * y
            z = source(j - 1) + m[j, zs, :] * z
        c_left, c_right, c_mid = p[mid - 1, zs, :], p[mid, zs, :], m[mid, zs, :]
        y, z = c_left * y + c_mid * z, c_right * z + c_mid * y
        for i in range(mid - 1, -1, -1):
            j = nx - 1 - i
            if i < mid - 1:
                y = ys[i] + m[i, zs, :] * y
                z = ys[j] + m[j, zs, :] * z
            b[i, zs, :], b[j, zs, :] = y, z


def y_pivots(kt, my, py):
    ny = kt.shape[0] // 8
    half = ny // 2

    def both(i, state):
        s, t, k_left, k_right = state
        j = ny - 1 - i
        next_left, next_right = row(kt, i + 1), row(kt, j - 1)
        e = 0.5 * (k_left + next_left)
        f = 0.5 * (k_right + next_right)
        inv_e = 1.0 / (s + e)
        inv_f = 1.0 / (t + f)
        m_left, m_right = e * inv_e, f * inv_f
        put(py, i, inv_e)
        put(py, j, inv_f)
        put(my, i, m_left)
        put(my, j, m_right)
        return 1.0 + s * m_left, 1.0 + t * m_right, next_left, next_right

    one = jnp.ones((8, 128), F32)
    s, t, k_left, k_right = lax.fori_loop(
        0, half - 1, both, (one, one, row(kt, 0), row(kt, ny - 1)), unroll=7
    )
    e = 0.5 * (k_left + k_right)
    inv = 1.0 / (s * t + e * (s + t))
    put(py, half - 1, (t + e) * inv)
    put(py, half, (s + e) * inv)
    put(my, half - 1, e * inv)
    put(my, half, e * inv)


def y_pivots_kernel(nx, k, ready, my, py, kt):
    for b in range(8):
        turn([tile(k, nx, b, x) for x in range(nx)], kt, b)
    y_pivots(kt, my, py)


def y_columns_kernel(nx, k, g0, gl, kt, m, p):
    for b in range(8):
        turn([tile(k, nx, b, x) for x in range(nx)], kt, b)
    y_pivots(kt, m, p)
    ny = kt.shape[0] // 8
    half = ny // 2
    w = x = jnp.ones((8, 128), F32)
    for i in range(half - 1):
        j = ny - 1 - i
        put(g0, i, w * row(p, i))
        put(gl, j, x * row(p, j))
        w, x = w * row(m, i), x * row(m, j)
    c_left, c_right, c_mid = row(p, half - 1), row(p, half), row(m, half)
    g_left, g_right = c_left * w, c_mid * w
    h_left, h_right = c_mid * x, c_right * x
    for i in range(half - 1, -1, -1):
        j = ny - 1 - i
        if i < half - 1:
            m_left, m_right = row(m, i), row(m, j)
            g_left, h_left = row(g0, i) + m_left * g_left, m_left * h_left
            g_right, h_right = m_right * g_right, row(gl, j) + m_right * h_right
        put(g0, i, g_left)
        put(g0, j, g_right)
        put(gl, i, h_left)
        put(gl, j, h_right)


def y_inner_kernel(dt, m, p, b):
    ny = dt.shape[0] // 8
    half = ny // 2
    y, z = row(dt, 0), row(dt, ny - 1)
    for i in range(half - 1):
        j = ny - 1 - i
        put(b, i, y * row(p, i))
        put(b, j, z * row(p, j))
        y = row(dt, i + 1) + row(m, i) * y
        z = row(dt, j - 1) + row(m, j) * z
    c_left, c_right, c_mid = row(p, half - 1), row(p, half), row(m, half)
    y, z = c_left * y + c_mid * z, c_right * z + c_mid * y
    for i in range(half - 1, -1, -1):
        j = ny - 1 - i
        if i < half - 1:
            y = row(b, i) + row(m, i) * y
            z = row(b, j) + row(m, j) * z
        put(b, i, y)
        put(b, j, z)


def solve(low, diag, up, rhs):
    n = len(diag)
    mid = n // 2
    c, q = [None] * n, [None] * n
    for order, near, far in (
        (range(mid), low, up),
        (range(n - 1, mid, -1), up, low),
    ):
        last = None
        for i in order:
            if last is None:
                inv = 1.0 / diag[i]
                q[i] = rhs[i] * inv
            else:
                inv = 1.0 / (diag[i] - near[i] * c[last])
                q[i] = (rhs[i] + near[i] * q[last]) * inv
            c[i] = far[i] * inv
            last = i
    i = mid
    inv = 1.0 / (diag[i] - low[i] * c[i - 1] - up[i] * c[i + 1])
    q[i] = (rhs[i] + low[i] * q[i - 1] + up[i] * q[i + 1]) * inv
    for i in range(mid - 1, -1, -1):
        q[i] = q[i] + c[i] * q[i + 1]
    for i in range(mid + 1, n):
        q[i] = q[i] + c[i] * q[i - 1]
    return q


def far_first(group):
    return [0] + [1, 3, 2]


def system(blocks, nothing):
    low, diag, up, rhs = [], [], [], []
    for before, after in zip([nothing] + blocks, blocks + [nothing]):
        e = 0.5 * (before[6] + after[5])
        low.append(e * before[1])
        diag.append(1.0 + e * (before[2] + after[0]))
        up.append(e * after[1])
        rhs.append(e * (after[3] - before[4]))
    return low, diag, up, rhs


def merge_kernel(group, *refs):
    got, sup, inner, recv = refs[:group], refs[group], refs[group + 1], refs[group + 2]
    own = sup.shape[0] // 7
    mine = lax.rem(lax.axis_index("row"), group)
    for step, ref in zip(far_first(group), got):
        recv[lax.rem(mine + group - step, group)] = ref[...]
    blocks = [tuple(recv[d, q * own : (q + 1) * own, :] for q in range(7)) for d in range(group)]
    low, diag, up, rhs = system(blocks, blocks[0])
    low, diag, up, rhs = low[1:group], diag[1:group], up[1:group], rhs[1:group]
    inv = 1.0 / diag[0]
    c_first, a_first, b_first = up[0] * inv, rhs[0] * inv, low[0] * inv
    inv = 1.0 / diag[2]
    c_last, a_last, g_last = low[2] * inv, rhs[2] * inv, up[2] * inv
    inv = 1.0 / (diag[1] - low[1] * c_first - up[1] * c_last)
    a_mid = (rhs[1] + low[1] * a_first + up[1] * a_last) * inv
    b_mid = low[1] * b_first * inv
    g_mid = up[1] * g_last * inv
    a_first, b_first, g_first = a_first + c_first * a_mid, b_first + c_first * b_mid, c_first * g_mid
    a_last, b_last, g_last = a_last + c_last * a_mid, c_last * b_mid, g_last + c_last * g_mid
    first, last = blocks[0], blocks[group - 1]
    parts = [
        first[0] - first[1] * b_first,
        first[1] * g_first,
        last[2] - last[1] * g_last,
        first[3] + first[1] * a_first,
        last[4] - last[1] * a_last,
        first[5],
        last[6],
    ]
    for q, part in enumerate(parts):
        sup[q * own : (q + 1) * own, :] = part
    kept = [a_first, a_mid, a_last, b_first, b_mid, b_last, g_first, g_mid, g_last]
    for q, part in enumerate(kept):
        inner[q * own : (q + 1) * own, :] = part


def flux_kernel(group, *refs):
    got, inner, sends = refs[:group], refs[group], refs[group + 3 : 2 * group + 3]
    recv, flux, send = refs[2 * group + 3 :]
    own = got[0].shape[0] // 7
    row_index = lax.axis_index("row")
    mine, outer = lax.rem(row_index, group), lax.div(row_index, group)
    for step, ref in zip(far_first(group), got):
        recv[lax.rem(outer + group - step, group)] = ref[...]
    blocks = [tuple(recv[d, q * own : (q + 1) * own, :] for q in range(7)) for d in range(group)]
    q = solve(*system(blocks, (jnp.zeros((own, 128), F32),) * 7))
    for i in range(group + 1):
        flux[i] = q[i]
    left, right = flux[outer], flux[outer + 1]

    def kept(i):
        return inner[i * own : (i + 1) * own, :]

    q = [left]
    for i in range(group - 1):
        q.append(kept(i) + kept(group - 1 + i) * left + kept(2 * group - 2 + i) * right)
    q.append(right)
    for d in range(group):
        send[d, 0:own, :] = q[d]
        send[d, own : 2 * own, :] = q[d + 1]
    for step, out in enumerate(sends):
        out[...] = send[lax.rem(mine + step, group)]


def y_send_kernel(nx, group, *refs):
    got = refs[:group]
    bx, g0x, glx, u, g0, gl, faces, send, dt, ql, qr = refs[group:]
    own = got[0].shape[0] // 2
    ny = dt.shape[0] // 8
    mine = lax.rem(lax.axis_index("row"), group)
    for step, ref in zip(far_first(group), got):
        start = pl.multiple_of(lax.rem(mine + group - step, group) * own, own)
        ql[pl.ds(start, own), :] = ref[0:own, :]
        qr[pl.ds(start, own), :] = ref[own : 2 * own, :]
    for t in range(8):
        zs = slice(t * 8, t * 8 + 8)
        left, right = ql[zs, :], qr[zs, :]
        turn(
            [
                (bx[i, zs, :] - tile(u, nx, t, i))
                + (glx[i, zs, :] * right - g0x[i, zs, :] * left)
                for i in range(nx)
            ],
            dt,
            t,
        )

    zero = jnp.zeros((8, 128), F32)
    b0, bl = [zero] * 4, [zero] * 4
    for j in range(ny):
        dj = row(dt, j)
        b0[j % 4] = b0[j % 4] + row(g0, j) * dj
        bl[j % 4] = bl[j % 4] + row(gl, j) * dj
    root_left, root_right = faces[0:8, :], faces[8:16, :]
    parts = [
        root_left * root_left * row(g0, 0),
        root_left * root_right * row(g0, ny - 1),
        root_right * root_right * row(gl, ny - 1),
        root_left * ((b0[0] + b0[1]) + (b0[2] + b0[3])),
        root_right * ((bl[0] + bl[1]) + (bl[2] + bl[3])),
    ]
    for q, part in enumerate(parts):
        send[q * 8 : (q + 1) * 8, :] = part


def join_kernel(mine, other, sup, mid):
    even = lax.rem(lax.axis_index("col"), 2) == 0
    first, second = [], []
    for q in range(5):
        here, there = mine[q * 8 : q * 8 + 8, :], other[q * 8 : q * 8 + 8, :]
        first.append(jnp.where(even, here, there))
        second.append(jnp.where(even, there, here))
    inv = 1.0 / (1.0 + (first[2] + second[0]))
    f = (second[3] - first[4]) * inv
    g, h = first[1] * inv, second[1] * inv
    parts = [
        first[0] - first[1] * g,
        first[1] * h,
        second[2] - second[1] * h,
        first[3] + first[1] * f,
        second[4] - second[1] * f,
    ]
    for q, part in enumerate(parts):
        sup[q * 8 : q * 8 + 8, :] = part
    for q, part in enumerate((f, g, h)):
        mid[q * 8 : q * 8 + 8, :] = part


def finish_kernel(nx, steps, *refs):
    peers = len(steps)
    got = refs[:peers]
    mid, b, g0, gl, u, faces, out, recv, flux, whole, done, sems = refs[peers:]
    col = lax.axis_index("col")
    chip = lax.div(col, 2)
    for step, ref in zip(steps, got):
        recv[lax.rem(chip + peers - step, peers)] = ref[...]
    nothing = (jnp.zeros((8, 128), F32),) * 5
    low, diag, up, rhs = [], [], [], []
    before = nothing
    for i in range(peers + 1):
        after = nothing
        if i < peers:
            after = tuple(recv[i, q * 8 : (q + 1) * 8, :] for q in range(5))
        low.append(before[1])
        diag.append(1.0 + (before[2] + after[0]))
        up.append(after[1])
        rhs.append(after[3] - before[4])
        before = after
    q = solve(low, diag, up, rhs)
    for i in range(peers + 1):
        flux[i] = q[i]
    left, right = flux[chip], flux[chip + 1]
    inner = mid[0:8, :] + mid[8:16, :] * left + mid[16:24, :] * right
    even = lax.rem(col, 2) == 0
    left, right = jnp.where(even, left, inner), jnp.where(even, inner, right)
    left = left * faces[0:8, :]
    right = right * faces[8:16, :]
    for j in range(b.shape[0] // 8):
        put(whole, j, row(b, j) + (row(gl, j) * right - row(g0, j) * left))
    copies = []
    for i in range(8):
        delta = turn_back(whole, i)
        for x in range(nx):
            done[pl.ds(i * 128 + x, 8, stride=nx), :] = delta[x * 8 : x * 8 + 8, :]
        span = slice(i * 128, (i + 1) * 128)
        done[span, :] = u[span, :] + done[span, :]
        rows = pl.ds(i * 128, 128)
        copy = pltpu.make_async_copy(done.at[rows], out.at[rows], sems.at[i])
        copy.start()
        copies.append(copy)
    for copy in copies:
        copy.wait()


def on_device(field, conductivity):
    nz, nx, ny = field.shape
    rows = nz * nx
    rowp, colp = lax.axis_size("row"), lax.axis_size("col")
    u = field.reshape(rows, ny)
    k = conductivity.reshape(rows, ny)
    flat, cube = (rows, ny), (nx, nz, ny)
    uv, kv, ut, kt, low, high = call(
        functools.partial(load_kernel, nx),
        [flat] * 4 + [(16, 128)] * 2,
        tuple(pltpu.with_memory_space_constraint(a, pltpu.HBM) for a in (u, k)),
        1 << 20,
        [pltpu.SemaphoreType.DMA((2,))],
        [HBM, HBM],
    )
    up = [(i, (i + 1) % colp) for i in range(colp)]
    from_left = lax.ppermute(high, "col", up)
    from_right = lax.ppermute(low, "col", [(b, a) for a, b in up])
    mx, px, g0x, glx, r, ends = call(
        functools.partial(pivots_kernel, nx),
        [cube] * 4 + [flat, (2, nz, ny)],
        (uv, kv, ut, kt),
        1 << 23,
        [flat, flat],
    )
    group = math.isqrt(rowp)
    own = nz // group
    inside, across = {}, {}
    for step in range(group):
        inside[step] = [(i, i // group * group + (i + step) % group) for i in range(rowp)]
        across[step] = [(i, (i + step * group) % rowp) for i in range(rowp)]

    def exchange(arrays, pairs):
        return [
            lax.ppermute(arrays[step], "row", pairs[step]) if step else arrays[0]
            for step in far_first(group)
        ]

    *parts, full, faces = call(
        functools.partial(x_send_kernel, nx, colp, group),
        [(7 * own, ny)] * group + [flat, (16, 128)],
        (low, high, from_left, from_right, r, ends, g0x, glx),
        1 << 22,
        [(128, 128), (group, 7 * own, ny)],
    )
    parts = exchange(parts, inside)
    (bx,) = call(functools.partial(x_inner_kernel, nx), [cube], (full, mx, px), 1 << 21)
    g0y, gly = call(functools.partial(y_columns_kernel, nx), [flat] * 2, (k,), 1 << 23, [flat] * 3)
    merged, inner = call(
        functools.partial(merge_kernel, group),
        [(7 * own, ny), (9 * own, ny)],
        parts,
        1 << 20,
        [(group, 7 * own, ny)],
    )
    parts = exchange([merged] * group, across)
    parts = call(
        functools.partial(flux_kernel, group),
        [(2 * own, ny)] * group,
        (*parts, inner, bx, g0y),
        1 << 20,
        [(group, 7 * own, ny), (group + 1, own, ny), (group, 2 * own, ny)],
    )
    parts = exchange(parts, inside)
    send, dt = call(
        functools.partial(y_send_kernel, nx, group),
        [(40, 128), flat],
        (*parts, bx, g0x, glx, u, g0y, gly, faces),
        1 << 22,
        [(nz, ny), (nz, ny)],
    )
    my, py = call(functools.partial(y_pivots_kernel, nx), [flat] * 2, (k, send), 1 << 22, [flat])
    (b,) = call(y_inner_kernel, [flat], (dt, my, py), 1 << 22)
    other = lax.ppermute(send, "col", [(i, i ^ 1) for i in range(colp)])
    sup, mid = call(join_kernel, [(40, 128), (24, 128)], (send, other), 1 << 16)
    chips = colp // 2
    steps = [0, 2, 1, 3]
    got = [
        lax.ppermute(sup, "col", [(i, (i + 2 * step) % colp) for i in range(colp)]) if step else sup
        for step in steps
    ]
    (out,) = call(
        functools.partial(finish_kernel, nx, steps),
        [flat],
        (*got, mid, b, g0y, gly, u, faces),
        1 << 22,
        [(chips, 40, 128), (chips + 1, 8, 128), flat, flat, pltpu.SemaphoreType.DMA((8,))],
        out_specs=[HBM],
    )
    return out.reshape(nz, nx, ny)


def solution(mesh):
    in_specs = (P(None, "row", "col"), P(None, "row", "col"))
    out_specs = P(None, "row", "col")
    return jax.shard_map(
        on_device, mesh=mesh, in_specs=in_specs, out_specs=out_specs, check_vma=False
    )
```

```python
import functools
import math

import jax
import jax.numpy as jnp
from jax import lax
from jax.experimental import pallas as pl
from jax.experimental.pallas import tpu as pltpu
from jax.sharding import PartitionSpec as P

z_weight = 0.02
F32 = jnp.float32
VMEM = pl.BlockSpec(memory_space=pltpu.VMEM)
HBM = pl.BlockSpec(memory_space=pltpu.HBM)


def call(kernel, outs, args, flops, scratch=(), specs=None, out_specs=None):
    return pl.pallas_call(
        kernel,
        out_shape=[jax.ShapeDtypeStruct(s, F32) for s in outs],
        in_specs=specs or [VMEM] * len(args),
        out_specs=out_specs or [VMEM] * len(outs),
        scratch_shapes=[pltpu.VMEM(s, F32) if isinstance(s, tuple) else s for s in scratch],
        compiler_params=pltpu.CompilerParams(vmem_limit_bytes=12 << 20),
        cost_estimate=pl.CostEstimate(flops=flops, bytes_accessed=1 << 20, transcendentals=0),
    )(*args)


def row(ref, j):
    start = j * 8 if isinstance(j, int) else pl.multiple_of(j * 8, 8)
    return ref[pl.ds(start, 8), :]


def put(ref, j, value):
    start = j * 8 if isinstance(j, int) else pl.multiple_of(j * 8, 8)
    ref[pl.ds(start, 8), :] = value


def tile(ref, nx, b, x):
    return ref[pl.ds(b * 8 * nx + x, 8, stride=nx), :]


def turn(tiles, target, b):
    target[pl.ds(b, 128, stride=8), :] = jnp.concatenate(tiles, axis=0).T


def turn_back(source, b):
    return source[pl.ds(b, 128, stride=8), :].T


def load_kernel(nx, u_hbm, k_hbm, u, k, ut, kt, low, high, sems):
    copies = [
        pltpu.make_async_copy(k_hbm, k, sems.at[0]),
        pltpu.make_async_copy(u_hbm, u, sems.at[1]),
    ]
    for copy in copies:
        copy.start()
    for copy, src, dst in zip(copies, (k, u), (kt, ut)):
        copy.wait()
        for b in range(8):
            turn([tile(src, nx, b, x) for x in range(nx)], dst, b)
    n = kt.shape[0] // 8
    low[0:8, :] = row(kt, 0)
    low[8:16, :] = row(ut, 0)
    high[0:8, :] = row(kt, n - 1)
    high[8:16, :] = row(ut, n - 1)


def pivots_kernel(nx, u, k, ut, kt, mx, px, g0, gl, r, ends, lt, rz):
    rows = u.shape[0]
    nz = rows // nx
    ny = lt.shape[0] // 8

    here_k, here_u = row(kt, 0), row(ut, 0)
    before = None
    for j in range(ny):
        if j + 1 < ny:
            next_k, next_u = row(kt, j + 1), row(ut, j + 1)
            flux = 0.5 * (here_k + next_k) * (next_u - here_u)
            put(lt, j, flux if before is None else flux - before)
            before, here_k, here_u = flux, next_k, next_u
        else:
            put(lt, j, -before)

    def at(ref, z):
        return ref[z * nx : (z + 1) * nx, :]

    uz, kz = at(u, 0), at(k, 0)
    below = (0.5 * z_weight) * kz * uz
    for z in range(nz):
        if z + 1 < nz:
            un, kn = at(u, z + 1), at(k, z + 1)
            above = (0.5 * z_weight) * (kz + kn) * (un - uz)
        else:
            un = kn = None
            above = -(0.5 * z_weight) * kz * uz
        rz[z * nx : (z + 1) * nx, :] = uz + (above - below)
        uz, kz, below = un, kn, above
    for b in range(8):
        side = turn_back(lt, b)
        for x in range(nx):
            start = (b * nx + x) * 8
            r[start : start + 8, :] = tile(rz, nx, b, x) + side[x * 8 : x * 8 + 8, :]

    def kx(i):
        return k[pl.ds(i, nz, stride=nx), :]

    mid = nx // 2
    s = t = jnp.ones((nz, 128), F32)
    k_left, k_right = kx(0), kx(nx - 1)
    ends[0] = k_left
    ends[1] = k_right
    for i in range(mid - 1):
        j = nx - 1 - i
        next_left, next_right = kx(i + 1), kx(j - 1)
        e = 0.5 * (k_left + next_left)
        f = 0.5 * (k_right + next_right)
        inv_e = 1.0 / (s + e)
        inv_f = 1.0 / (t + f)
        m_left, m_right = e * inv_e, f * inv_f
        px[i], px[j] = inv_e, inv_f
        mx[i], mx[j] = m_left, m_right
        s, t = 1.0 + s * m_left, 1.0 + t * m_right
        k_left, k_right = next_left, next_right
    e = 0.5 * (k_left + k_right)
    inv = 1.0 / (s * t + e * (s + t))
    c_left, c_right, c_mid = (t + e) * inv, (s + e) * inv, e * inv
    px[mid - 1], px[mid] = c_left, c_right
    mx[mid - 1] = mx[mid] = c_mid
    w = v = jnp.ones((nz, 128), F32)
    for i in range(mid - 1):
        j = nx - 1 - i
        g0[i], gl[j] = w * px[i], v * px[j]
        w, v = w * mx[i], v * mx[j]
    g_left, g_right = c_left * w, c_mid * w
    h_left, h_right = c_mid * v, c_right * v
    for i in range(mid - 1, -1, -1):
        j = nx - 1 - i
        if i < mid - 1:
            m_left, m_right = mx[i], mx[j]
            g_left, h_left = g0[i] + m_left * g_left, m_left * h_left
            g_right, h_right = m_right * g_right, gl[j] + m_right * h_right
        g0[i], g0[j] = g_left, g_right
        gl[i], gl[j] = h_left, h_right


def x_send_kernel(nx, peers_y, group, low, high, from_left, from_right, r, ends, g0, gl, *refs):
    sends = refs[:group]
    full, faces, turned, send = refs[group:]
    rows = r.shape[0]
    nz = rows // nx
    col = lax.axis_index("col")
    left = jnp.where(col == 0, 0.0, from_left[...])
    right = jnp.where(col == peers_y - 1, 0.0, from_right[...])
    k_low, u_low = low[0:8, :], low[8:16, :]
    k_high, u_high = high[0:8, :], high[8:16, :]
    face_left = 0.5 * (k_low + left[0:8, :])
    face_right = 0.5 * (k_high + right[0:8, :])
    faces[0:8, :] = jnp.sqrt(face_left)
    faces[8:16, :] = jnp.sqrt(face_right)
    turned[0:8, :] = face_left * (left[8:16, :] - u_low)
    turned[8:16, :] = face_right * (right[8:16, :] - u_high)
    turned[16:128, :] = jnp.zeros((112, 128), F32)
    corr = turned[...].T
    lane = lax.broadcasted_iota(jnp.int32, (128, 128), 1)
    own = nz // group
    for t in range(8):
        zs = slice(t * 8, t * 8 + 8)
        west = jnp.where(lane == 0, corr[:, t : t + 1], 0.0)
        both = jnp.where(lane == 127, corr[:, 8 + t : 9 + t], west)

        zero = jnp.zeros((8, 128), F32)
        b0, bl = [zero, zero], [zero, zero]
        for i in range(nx):
            start = (t * nx + i) * 8
            ri = r[start : start + 8, :] + both[i * 8 : i * 8 + 8, :]
            full[start : start + 8, :] = ri
            b0[i % 2] = b0[i % 2] + g0[i, zs, :] * ri
            bl[i % 2] = bl[i % 2] + gl[i, zs, :] * ri
        parts = [
            g0[0, zs, :],
            g0[nx - 1, zs, :],
            gl[nx - 1, zs, :],
            b0[0] + b0[1],
            bl[0] + bl[1],
            ends[0, zs, :],
            ends[1, zs, :],
        ]
        for q, part in enumerate(parts):
            start = q * own + t * 8 % own
            send[t * 8 // own, start : start + 8, :] = part
    mine = lax.rem(lax.axis_index("row"), group)
    for step, out in enumerate(sends):
        out[...] = send[lax.rem(mine + step, group)]


def x_inner_kernel(nx, r, m, p, b):
    mid = nx // 2
    for t in range(8):
        zs = slice(t * 8, t * 8 + 8)

        def source(i):
            start = (t * nx + i) * 8
            return r[start : start + 8, :]

        ys = {}
        y, z = source(0), source(nx - 1)
        for i in range(mid - 1):
            j = nx - 1 - i
            ys[i], ys[j] = y * p[i, zs, :], z * p[j, zs, :]
            y = source(i + 1) + m[i, zs, :] * y
            z = source(j - 1) + m[j, zs, :] * z
        c_left, c_right, c_mid = p[mid - 1, zs, :], p[mid, zs, :], m[mid, zs, :]
        y, z = c_left * y + c_mid * z, c_right * z + c_mid * y
        for i in range(mid - 1, -1, -1):
            j = nx - 1 - i
            if i < mid - 1:
                y = ys[i] + m[i, zs, :] * y
                z = ys[j] + m[j, zs, :] * z
            b[i, zs, :], b[j, zs, :] = y, z


def y_pivots(kt, my, py):
    ny = kt.shape[0] // 8
    half = ny // 2

    def both(i, state):
        s, t, k_left, k_right = state
        j = ny - 1 - i
        next_left, next_right = row(kt, i + 1), row(kt, j - 1)
        e = 0.5 * (k_left + next_left)
        f = 0.5 * (k_right + next_right)
        inv_e = 1.0 / (s + e)
        inv_f = 1.0 / (t + f)
        m_left, m_right = e * inv_e, f * inv_f
        put(py, i, inv_e)
        put(py, j, inv_f)
        put(my, i, m_left)
        put(my, j, m_right)
        return 1.0 + s * m_left, 1.0 + t * m_right, next_left, next_right

    one = jnp.ones((8, 128), F32)
    s, t, k_left, k_right = lax.fori_loop(
        0, half - 1, both, (one, one, row(kt, 0), row(kt, ny - 1)), unroll=7
    )
    e = 0.5 * (k_left + k_right)
    inv = 1.0 / (s * t + e * (s + t))
    put(py, half - 1, (t + e) * inv)
    put(py, half, (s + e) * inv)
    put(my, half - 1, e * inv)
    put(my, half, e * inv)


def y_pivots_kernel(nx, k, ready, my, py, kt):
    for b in range(8):
        turn([tile(k, nx, b, x) for x in range(nx)], kt, b)
    y_pivots(kt, my, py)


def y_columns_kernel(nx, k, g0, gl, kt, m, p):
    for b in range(8):
        turn([tile(k, nx, b, x) for x in range(nx)], kt, b)
    y_pivots(kt, m, p)
    ny = kt.shape[0] // 8
    half = ny // 2
    w = x = jnp.ones((8, 128), F32)
    for i in range(half - 1):
        j = ny - 1 - i
        put(g0, i, w * row(p, i))
        put(gl, j, x * row(p, j))
        w, x = w * row(m, i), x * row(m, j)
    c_left, c_right, c_mid = row(p, half - 1), row(p, half), row(m, half)
    g_left, g_right = c_left * w, c_mid * w
    h_left, h_right = c_mid * x, c_right * x
    for i in range(half - 1, -1, -1):
        j = ny - 1 - i
        if i < half - 1:
            m_left, m_right = row(m, i), row(m, j)
            g_left, h_left = row(g0, i) + m_left * g_left, m_left * h_left
            g_right, h_right = m_right * g_right, row(gl, j) + m_right * h_right
        put(g0, i, g_left)
        put(g0, j, g_right)
        put(gl, i, h_left)
        put(gl, j, h_right)


def y_inner_kernel(dt, m, p, b):
    ny = dt.shape[0] // 8
    half = ny // 2
    y, z = row(dt, 0), row(dt, ny - 1)
    for i in range(half - 1):
        j = ny - 1 - i
        put(b, i, y * row(p, i))
        put(b, j, z * row(p, j))
        y = row(dt, i + 1) + row(m, i) * y
        z = row(dt, j - 1) + row(m, j) * z
    c_left, c_right, c_mid = row(p, half - 1), row(p, half), row(m, half)
    y, z = c_left * y + c_mid * z, c_right * z + c_mid * y
    for i in range(half - 1, -1, -1):
        j = ny - 1 - i
        if i < half - 1:
            y = row(b, i) + row(m, i) * y
            z = row(b, j) + row(m, j) * z
        put(b, i, y)
        put(b, j, z)


def solve(low, diag, up, rhs):
    n = len(diag)
    mid = n // 2
    c, q = [None] * n, [None] * n
    for order, near, far in (
        (range(mid), low, up),
        (range(n - 1, mid, -1), up, low),
    ):
        last = None
        for i in order:
            if last is None:
                inv = 1.0 / diag[i]
                q[i] = rhs[i] * inv
            else:
                inv = 1.0 / (diag[i] - near[i] * c[last])
                q[i] = (rhs[i] + near[i] * q[last]) * inv
            c[i] = far[i] * inv
            last = i
    i = mid
    inv = 1.0 / (diag[i] - low[i] * c[i - 1] - up[i] * c[i + 1])
    q[i] = (rhs[i] + low[i] * q[i - 1] + up[i] * q[i + 1]) * inv
    for i in range(mid - 1, -1, -1):
        q[i] = q[i] + c[i] * q[i + 1]
    for i in range(mid + 1, n):
        q[i] = q[i] + c[i] * q[i - 1]
    return q


def shift_order(group):
    return [1, 3, 2, 0]


def system(blocks, nothing):
    low, diag, up, rhs = [], [], [], []
    for before, after in zip([nothing] + blocks, blocks + [nothing]):
        e = 0.5 * (before[6] + after[5])
        low.append(e * before[1])
        diag.append(1.0 + e * (before[2] + after[0]))
        up.append(e * after[1])
        rhs.append(e * (after[3] - before[4]))
    return low, diag, up, rhs


def merge_kernel(group, *refs):
    got, sup, inner, recv = refs[:group], refs[group], refs[group + 1], refs[group + 2]
    own = sup.shape[0] // 7
    mine = lax.rem(lax.axis_index("row"), group)
    for step, ref in zip(shift_order(group), got):
        recv[lax.rem(mine + group - step, group)] = ref[...]
    blocks = [tuple(recv[d, q * own : (q + 1) * own, :] for q in range(7)) for d in range(group)]
    low, diag, up, rhs = system(blocks, blocks[0])
    low, diag, up, rhs = low[1:group], diag[1:group], up[1:group], rhs[1:group]
    inv = 1.0 / diag[0]
    c_first, a_first, b_first = up[0] * inv, rhs[0] * inv, low[0] * inv
    inv = 1.0 / diag[2]
    c_last, a_last, g_last = low[2] * inv, rhs[2] * inv, up[2] * inv
    inv = 1.0 / (diag[1] - low[1] * c_first - up[1] * c_last)
    a_mid = (rhs[1] + low[1] * a_first + up[1] * a_last) * inv
    b_mid = low[1] * b_first * inv
    g_mid = up[1] * g_last * inv
    a_first, b_first, g_first = a_first + c_first * a_mid, b_first + c_first * b_mid, c_first * g_mid
    a_last, b_last, g_last = a_last + c_last * a_mid, c_last * b_mid, g_last + c_last * g_mid
    first, last = blocks[0], blocks[group - 1]
    parts = [
        first[0] - first[1] * b_first,
        first[1] * g_first,
        last[2] - last[1] * g_last,
        first[3] + first[1] * a_first,
        last[4] - last[1] * a_last,
        first[5],
        last[6],
    ]
    for q, part in enumerate(parts):
        sup[q * own : (q + 1) * own, :] = part
    kept = [a_first, a_mid, a_last, b_first, b_mid, b_last, g_first, g_mid, g_last]
    for q, part in enumerate(kept):
        inner[q * own : (q + 1) * own, :] = part


def flux_kernel(group, *refs):
    got, inner, sends = refs[:group], refs[group], refs[group + 3 : 2 * group + 3]
    recv, flux, send = refs[2 * group + 3 :]
    own = got[0].shape[0] // 7
    row_index = lax.axis_index("row")
    mine, outer = lax.rem(row_index, group), lax.div(row_index, group)
    for step, ref in zip(shift_order(group), got):
        recv[lax.rem(outer + group - step, group)] = ref[...]
    blocks = [tuple(recv[d, q * own : (q + 1) * own, :] for q in range(7)) for d in range(group)]
    q = solve(*system(blocks, (jnp.zeros((own, 128), F32),) * 7))
    for i in range(group + 1):
        flux[i] = q[i]
    left, right = flux[outer], flux[outer + 1]

    def kept(i):
        return inner[i * own : (i + 1) * own, :]

    q = [left]
    for i in range(group - 1):
        q.append(kept(i) + kept(group - 1 + i) * left + kept(2 * group - 2 + i) * right)
    q.append(right)
    for d in range(group):
        send[d, 0:own, :] = q[d]
        send[d, own : 2 * own, :] = q[d + 1]
    for step, out in enumerate(sends):
        out[...] = send[lax.rem(mine + step, group)]


def y_send_kernel(nx, group, *refs):
    got = refs[:group]
    bx, g0x, glx, u, g0, gl, faces, send, dt, ql, qr = refs[group:]
    own = got[0].shape[0] // 2
    ny = dt.shape[0] // 8
    mine = lax.rem(lax.axis_index("row"), group)
    for step, ref in zip(shift_order(group), got):
        start = pl.multiple_of(lax.rem(mine + group - step, group) * own, own)
        ql[pl.ds(start, own), :] = ref[0:own, :]
        qr[pl.ds(start, own), :] = ref[own : 2 * own, :]
    for t in range(8):
        zs = slice(t * 8, t * 8 + 8)
        left, right = ql[zs, :], qr[zs, :]
        turn(
            [
                (bx[i, zs, :] - tile(u, nx, t, i))
                + (glx[i, zs, :] * right - g0x[i, zs, :] * left)
                for i in range(nx)
            ],
            dt,
            t,
        )

    zero = jnp.zeros((8, 128), F32)
    b0, bl = [zero] * 4, [zero] * 4
    for j in range(ny):
        dj = row(dt, j)
        b0[j % 4] = b0[j % 4] + row(g0, j) * dj
        bl[j % 4] = bl[j % 4] + row(gl, j) * dj
    root_left, root_right = faces[0:8, :], faces[8:16, :]
    parts = [
        root_left * root_left * row(g0, 0),
        root_left * root_right * row(g0, ny - 1),
        root_right * root_right * row(gl, ny - 1),
        root_left * ((b0[0] + b0[1]) + (b0[2] + b0[3])),
        root_right * ((bl[0] + bl[1]) + (bl[2] + bl[3])),
    ]
    for q, part in enumerate(parts):
        send[q * 8 : (q + 1) * 8, :] = part


def join_kernel(mine, other, sup, mid):
    even = lax.rem(lax.axis_index("col"), 2) == 0
    first, second = [], []
    for q in range(5):
        here, there = mine[q * 8 : q * 8 + 8, :], other[q * 8 : q * 8 + 8, :]
        first.append(jnp.where(even, here, there))
        second.append(jnp.where(even, there, here))
    inv = 1.0 / (1.0 + (first[2] + second[0]))
    f = (second[3] - first[4]) * inv
    g, h = first[1] * inv, second[1] * inv
    parts = [
        first[0] - first[1] * g,
        first[1] * h,
        second[2] - second[1] * h,
        first[3] + first[1] * f,
        second[4] - second[1] * f,
    ]
    for q, part in enumerate(parts):
        sup[q * 8 : q * 8 + 8, :] = part
    for q, part in enumerate((f, g, h)):
        mid[q * 8 : q * 8 + 8, :] = part


def finish_kernel(nx, steps, *refs):
    peers = len(steps)
    got = refs[:peers]
    mid, b, g0, gl, u, faces, out, recv, flux, whole, done, sems = refs[peers:]
    col = lax.axis_index("col")
    chip = lax.div(col, 2)
    for step, ref in zip(steps, got):
        recv[lax.rem(chip + peers - step, peers)] = ref[...]
    nothing = (jnp.zeros((8, 128), F32),) * 5
    low, diag, up, rhs = [], [], [], []
    before = nothing
    for i in range(peers + 1):
        after = nothing
        if i < peers:
            after = tuple(recv[i, q * 8 : (q + 1) * 8, :] for q in range(5))
        low.append(before[1])
        diag.append(1.0 + (before[2] + after[0]))
        up.append(after[1])
        rhs.append(after[3] - before[4])
        before = after
    q = solve(low, diag, up, rhs)
    for i in range(peers + 1):
        flux[i] = q[i]
    left, right = flux[chip], flux[chip + 1]
    inner = mid[0:8, :] + mid[8:16, :] * left + mid[16:24, :] * right
    even = lax.rem(col, 2) == 0
    left, right = jnp.where(even, left, inner), jnp.where(even, inner, right)
    left = left * faces[0:8, :]
    right = right * faces[8:16, :]
    for j in range(b.shape[0] // 8):
        put(whole, j, row(b, j) + (row(gl, j) * right - row(g0, j) * left))
    copies = []
    for i in range(8):
        delta = turn_back(whole, i)
        for x in range(nx):
            done[pl.ds(i * 128 + x, 8, stride=nx), :] = delta[x * 8 : x * 8 + 8, :]
        span = slice(i * 128, (i + 1) * 128)
        done[span, :] = u[span, :] + done[span, :]
        rows = pl.ds(i * 128, 128)
        copy = pltpu.make_async_copy(done.at[rows], out.at[rows], sems.at[i])
        copy.start()
        copies.append(copy)
    for copy in copies:
        copy.wait()


def on_device(field, conductivity):
    nz, nx, ny = field.shape
    rows = nz * nx
    rowp, colp = lax.axis_size("row"), lax.axis_size("col")
    u = field.reshape(rows, ny)
    k = conductivity.reshape(rows, ny)
    flat, cube = (rows, ny), (nx, nz, ny)
    uv, kv, ut, kt, low, high = call(
        functools.partial(load_kernel, nx),
        [flat] * 4 + [(16, 128)] * 2,
        tuple(pltpu.with_memory_space_constraint(a, pltpu.HBM) for a in (u, k)),
        1 << 20,
        [pltpu.SemaphoreType.DMA((2,))],
        [HBM, HBM],
    )
    up = [(i, (i + 1) % colp) for i in range(colp)]
    from_left = lax.ppermute(high, "col", up)
    from_right = lax.ppermute(low, "col", [(b, a) for a, b in up])
    mx, px, g0x, glx, r, ends = call(
        functools.partial(pivots_kernel, nx),
        [cube] * 4 + [flat, (2, nz, ny)],
        (uv, kv, ut, kt),
        1 << 23,
        [flat, flat],
    )
    group = math.isqrt(rowp)
    own = nz // group
    inside, across = {}, {}
    for step in range(group):
        inside[step] = [
            (i * colp + c, (i // group * group + (i + step) % group) * colp + (c ^ 1))
            for i in range(rowp)
            for c in range(colp)
        ]
        across[step] = [(i, (i + step * group) % rowp) for i in range(rowp)]

    def exchange(arrays, pairs, axes):
        return [
            lax.ppermute(arrays[step], axes, pairs[step]) if step or axes != "row" else arrays[0]
            for step in shift_order(group)
        ]

    *parts, full, faces = call(
        functools.partial(x_send_kernel, nx, colp, group),
        [(7 * own, ny)] * group + [flat, (16, 128)],
        (low, high, from_left, from_right, r, ends, g0x, glx),
        1 << 22,
        [(128, 128), (group, 7 * own, ny)],
    )
    parts = exchange(parts, inside, ("row", "col"))
    (bx,) = call(functools.partial(x_inner_kernel, nx), [cube], (full, mx, px), 1 << 21)
    g0y, gly = call(functools.partial(y_columns_kernel, nx), [flat] * 2, (k,), 1 << 23, [flat] * 3)
    merged, inner = call(
        functools.partial(merge_kernel, group),
        [(7 * own, ny), (9 * own, ny)],
        parts,
        1 << 20,
        [(group, 7 * own, ny)],
    )
    parts = exchange([merged] * group, across, "row")
    parts = call(
        functools.partial(flux_kernel, group),
        [(2 * own, ny)] * group,
        (*parts, inner, bx, g0y),
        1 << 20,
        [(group, 7 * own, ny), (group + 1, own, ny), (group, 2 * own, ny)],
    )
    parts = exchange(parts, inside, ("row", "col"))
    send, dt = call(
        functools.partial(y_send_kernel, nx, group),
        [(40, 128), flat],
        (*parts, bx, g0x, glx, u, g0y, gly, faces),
        1 << 22,
        [(nz, ny), (nz, ny)],
    )
    my, py = call(functools.partial(y_pivots_kernel, nx), [flat] * 2, (k, send), 1 << 22, [flat])
    (b,) = call(y_inner_kernel, [flat], (dt, my, py), 1 << 22)
    other = lax.ppermute(send, "col", [(i, i ^ 1) for i in range(colp)])
    sup, mid = call(join_kernel, [(40, 128), (24, 128)], (send, other), 1 << 16)
    chips = colp // 2
    steps = [0, 2, 1, 3]
    got = [
        lax.ppermute(sup, "col", [(i, (i + 2 * step) % colp) for i in range(colp)]) if step else sup
        for step in steps
    ]
    (out,) = call(
        functools.partial(finish_kernel, nx, steps),
        [flat],
        (*got, mid, b, g0y, gly, u, faces),
        1 << 22,
        [(chips, 40, 128), (chips + 1, 8, 128), flat, flat, pltpu.SemaphoreType.DMA((8,))],
        out_specs=[HBM],
    )
    return out.reshape(nz, nx, ny)


def solution(mesh):
    in_specs = (P(None, "row", "col"), P(None, "row", "col"))
    out_specs = P(None, "row", "col")
    return jax.shard_map(
        on_device, mesh=mesh, in_specs=in_specs, out_specs=out_specs, check_vma=False
    )
```

```python
import functools
import math

import jax
import jax.numpy as jnp
from jax import lax
from jax.experimental import pallas as pl
from jax.experimental.pallas import tpu as pltpu
from jax.sharding import PartitionSpec as P

z_weight = 0.02
F32 = jnp.float32
VMEM = pl.BlockSpec(memory_space=pltpu.VMEM)
HBM = pl.BlockSpec(memory_space=pltpu.HBM)


def call(kernel, outs, args, flops, scratch=(), specs=None, out_specs=None):
    return pl.pallas_call(
        kernel,
        out_shape=[jax.ShapeDtypeStruct(s, F32) for s in outs],
        in_specs=specs or [VMEM] * len(args),
        out_specs=out_specs or [VMEM] * len(outs),
        scratch_shapes=[pltpu.VMEM(s, F32) if isinstance(s, tuple) else s for s in scratch],
        compiler_params=pltpu.CompilerParams(vmem_limit_bytes=12 << 20),
        cost_estimate=pl.CostEstimate(flops=flops, bytes_accessed=1 << 20, transcendentals=0),
    )(*args)


def row(ref, j):
    start = j * 8 if isinstance(j, int) else pl.multiple_of(j * 8, 8)
    return ref[pl.ds(start, 8), :]


def put(ref, j, value):
    start = j * 8 if isinstance(j, int) else pl.multiple_of(j * 8, 8)
    ref[pl.ds(start, 8), :] = value


def tile(ref, nx, b, x):
    return ref[pl.ds(b * 8 * nx + x, 8, stride=nx), :]


def turn(tiles, target, b):
    target[pl.ds(b, 128, stride=8), :] = jnp.concatenate(tiles, axis=0).T


def turn_back(source, b):
    return source[pl.ds(b, 128, stride=8), :].T


def load_kernel(nx, u_hbm, k_hbm, u, k, ut, kt, low, high, sems):
    copies = [
        pltpu.make_async_copy(k_hbm, k, sems.at[0]),
        pltpu.make_async_copy(u_hbm, u, sems.at[1]),
    ]
    for copy in copies:
        copy.start()
    for copy, src, dst in zip(copies, (k, u), (kt, ut)):
        copy.wait()
        for b in range(8):
            turn([tile(src, nx, b, x) for x in range(nx)], dst, b)
    n = kt.shape[0] // 8
    low[0:8, :] = row(kt, 0)
    low[8:16, :] = row(ut, 0)
    high[0:8, :] = row(kt, n - 1)
    high[8:16, :] = row(ut, n - 1)


def pivots_kernel(nx, u, k, ut, kt, mx, px, g0, gl, r, ends, lt, rz):
    rows = u.shape[0]
    nz = rows // nx
    ny = lt.shape[0] // 8

    here_k, here_u = row(kt, 0), row(ut, 0)
    before = None
    for j in range(ny):
        if j + 1 < ny:
            next_k, next_u = row(kt, j + 1), row(ut, j + 1)
            flux = 0.5 * (here_k + next_k) * (next_u - here_u)
            put(lt, j, flux if before is None else flux - before)
            before, here_k, here_u = flux, next_k, next_u
        else:
            put(lt, j, -before)

    def at(ref, z):
        return ref[z * nx : (z + 1) * nx, :]

    uz, kz = at(u, 0), at(k, 0)
    below = (0.5 * z_weight) * kz * uz
    for z in range(nz):
        if z + 1 < nz:
            un, kn = at(u, z + 1), at(k, z + 1)
            above = (0.5 * z_weight) * (kz + kn) * (un - uz)
        else:
            un = kn = None
            above = -(0.5 * z_weight) * kz * uz
        rz[z * nx : (z + 1) * nx, :] = uz + (above - below)
        uz, kz, below = un, kn, above
    for b in range(8):
        side = turn_back(lt, b)
        for x in range(nx):
            start = (b * nx + x) * 8
            r[start : start + 8, :] = tile(rz, nx, b, x) + side[x * 8 : x * 8 + 8, :]

    def kx(i):
        return k[pl.ds(i, nz, stride=nx), :]

    mid = nx // 2
    s = t = jnp.ones((nz, 128), F32)
    k_left, k_right = kx(0), kx(nx - 1)
    ends[0] = k_left
    ends[1] = k_right
    for i in range(mid - 1):
        j = nx - 1 - i
        next_left, next_right = kx(i + 1), kx(j - 1)
        e = 0.5 * (k_left + next_left)
        f = 0.5 * (k_right + next_right)
        inv_e = 1.0 / (s + e)
        inv_f = 1.0 / (t + f)
        m_left, m_right = e * inv_e, f * inv_f
        px[i], px[j] = inv_e, inv_f
        mx[i], mx[j] = m_left, m_right
        s, t = 1.0 + s * m_left, 1.0 + t * m_right
        k_left, k_right = next_left, next_right
    e = 0.5 * (k_left + k_right)
    inv = 1.0 / (s * t + e * (s + t))
    c_left, c_right, c_mid = (t + e) * inv, (s + e) * inv, e * inv
    px[mid - 1], px[mid] = c_left, c_right
    mx[mid - 1] = mx[mid] = c_mid
    w = v = jnp.ones((nz, 128), F32)
    for i in range(mid - 1):
        j = nx - 1 - i
        g0[i], gl[j] = w * px[i], v * px[j]
        w, v = w * mx[i], v * mx[j]
    g_left, g_right = c_left * w, c_mid * w
    h_left, h_right = c_mid * v, c_right * v
    for i in range(mid - 1, -1, -1):
        j = nx - 1 - i
        if i < mid - 1:
            m_left, m_right = mx[i], mx[j]
            g_left, h_left = g0[i] + m_left * g_left, m_left * h_left
            g_right, h_right = m_right * g_right, gl[j] + m_right * h_right
        g0[i], g0[j] = g_left, g_right
        gl[i], gl[j] = h_left, h_right


def x_send_kernel(nx, peers_y, group, low, high, from_left, from_right, r, ends, g0, gl, *refs):
    sends = refs[:group]
    full, faces, turned, send = refs[group:]
    rows = r.shape[0]
    nz = rows // nx
    col = lax.axis_index("col")
    left = jnp.where(col == 0, 0.0, from_left[...])
    right = jnp.where(col == peers_y - 1, 0.0, from_right[...])
    k_low, u_low = low[0:8, :], low[8:16, :]
    k_high, u_high = high[0:8, :], high[8:16, :]
    face_left = 0.5 * (k_low + left[0:8, :])
    face_right = 0.5 * (k_high + right[0:8, :])
    faces[0:8, :] = jnp.sqrt(face_left)
    faces[8:16, :] = jnp.sqrt(face_right)
    turned[0:8, :] = face_left * (left[8:16, :] - u_low)
    turned[8:16, :] = face_right * (right[8:16, :] - u_high)
    turned[16:128, :] = jnp.zeros((112, 128), F32)
    corr = turned[...].T
    lane = lax.broadcasted_iota(jnp.int32, (128, 128), 1)
    own = nz // group
    for t in range(8):
        zs = slice(t * 8, t * 8 + 8)
        west = jnp.where(lane == 0, corr[:, t : t + 1], 0.0)
        both = jnp.where(lane == 127, corr[:, 8 + t : 9 + t], west)

        zero = jnp.zeros((8, 128), F32)
        b0, bl = [zero, zero], [zero, zero]
        for i in range(nx):
            start = (t * nx + i) * 8
            ri = r[start : start + 8, :] + both[i * 8 : i * 8 + 8, :]
            full[start : start + 8, :] = ri
            b0[i % 2] = b0[i % 2] + g0[i, zs, :] * ri
            bl[i % 2] = bl[i % 2] + gl[i, zs, :] * ri
        parts = [
            g0[0, zs, :],
            g0[nx - 1, zs, :],
            gl[nx - 1, zs, :],
            b0[0] + b0[1],
            bl[0] + bl[1],
            ends[0, zs, :],
            ends[1, zs, :],
        ]
        for q, part in enumerate(parts):
            start = q * own + t * 8 % own
            send[t * 8 // own, start : start + 8, :] = part
    mine = lax.rem(lax.axis_index("row"), group)
    for step, out in enumerate(sends):
        out[...] = send[lax.rem(mine + step, group)]


def x_inner_kernel(nx, r, m, p, b):
    mid = nx // 2
    for t in range(8):
        zs = slice(t * 8, t * 8 + 8)

        def source(i):
            start = (t * nx + i) * 8
            return r[start : start + 8, :]

        ys = {}
        y, z = source(0), source(nx - 1)
        for i in range(mid - 1):
            j = nx - 1 - i
            ys[i], ys[j] = y * p[i, zs, :], z * p[j, zs, :]
            y = source(i + 1) + m[i, zs, :] * y
            z = source(j - 1) + m[j, zs, :] * z
        c_left, c_right, c_mid = p[mid - 1, zs, :], p[mid, zs, :], m[mid, zs, :]
        y, z = c_left * y + c_mid * z, c_right * z + c_mid * y
        for i in range(mid - 1, -1, -1):
            j = nx - 1 - i
            if i < mid - 1:
                y = ys[i] + m[i, zs, :] * y
                z = ys[j] + m[j, zs, :] * z
            b[i, zs, :], b[j, zs, :] = y, z


def y_pivots(kt, my, py):
    ny = kt.shape[0] // 8
    half = ny // 2

    def both(i, state):
        s, t, k_left, k_right = state
        j = ny - 1 - i
        next_left, next_right = row(kt, i + 1), row(kt, j - 1)
        e = 0.5 * (k_left + next_left)
        f = 0.5 * (k_right + next_right)
        inv_e = 1.0 / (s + e)
        inv_f = 1.0 / (t + f)
        m_left, m_right = e * inv_e, f * inv_f
        put(py, i, inv_e)
        put(py, j, inv_f)
        put(my, i, m_left)
        put(my, j, m_right)
        return 1.0 + s * m_left, 1.0 + t * m_right, next_left, next_right

    one = jnp.ones((8, 128), F32)
    s, t, k_left, k_right = lax.fori_loop(
        0, half - 1, both, (one, one, row(kt, 0), row(kt, ny - 1)), unroll=7
    )
    e = 0.5 * (k_left + k_right)
    inv = 1.0 / (s * t + e * (s + t))
    put(py, half - 1, (t + e) * inv)
    put(py, half, (s + e) * inv)
    put(my, half - 1, e * inv)
    put(my, half, e * inv)


def y_pivots_kernel(nx, k, ready, my, py, kt):
    for b in range(8):
        turn([tile(k, nx, b, x) for x in range(nx)], kt, b)
    y_pivots(kt, my, py)


def y_columns_kernel(nx, k, g0, gl, kt, m, p):
    for b in range(8):
        turn([tile(k, nx, b, x) for x in range(nx)], kt, b)
    y_pivots(kt, m, p)
    ny = kt.shape[0] // 8
    half = ny // 2
    w = x = jnp.ones((8, 128), F32)
    for i in range(half - 1):
        j = ny - 1 - i
        put(g0, i, w * row(p, i))
        put(gl, j, x * row(p, j))
        w, x = w * row(m, i), x * row(m, j)
    c_left, c_right, c_mid = row(p, half - 1), row(p, half), row(m, half)
    g_left, g_right = c_left * w, c_mid * w
    h_left, h_right = c_mid * x, c_right * x
    for i in range(half - 1, -1, -1):
        j = ny - 1 - i
        if i < half - 1:
            m_left, m_right = row(m, i), row(m, j)
            g_left, h_left = row(g0, i) + m_left * g_left, m_left * h_left
            g_right, h_right = m_right * g_right, row(gl, j) + m_right * h_right
        put(g0, i, g_left)
        put(g0, j, g_right)
        put(gl, i, h_left)
        put(gl, j, h_right)


def y_inner_kernel(dt, m, p, b):
    ny = dt.shape[0] // 8
    half = ny // 2
    y, z = row(dt, 0), row(dt, ny - 1)
    for i in range(half - 1):
        j = ny - 1 - i
        put(b, i, y * row(p, i))
        put(b, j, z * row(p, j))
        y = row(dt, i + 1) + row(m, i) * y
        z = row(dt, j - 1) + row(m, j) * z
    c_left, c_right, c_mid = row(p, half - 1), row(p, half), row(m, half)
    y, z = c_left * y + c_mid * z, c_right * z + c_mid * y
    for i in range(half - 1, -1, -1):
        j = ny - 1 - i
        if i < half - 1:
            y = row(b, i) + row(m, i) * y
            z = row(b, j) + row(m, j) * z
        put(b, i, y)
        put(b, j, z)


def solve(low, diag, up, rhs):
    n = len(diag)
    mid = n // 2
    c, q = [None] * n, [None] * n
    for order, near, far in (
        (range(mid), low, up),
        (range(n - 1, mid, -1), up, low),
    ):
        last = None
        for i in order:
            if last is None:
                inv = 1.0 / diag[i]
                q[i] = rhs[i] * inv
            else:
                inv = 1.0 / (diag[i] - near[i] * c[last])
                q[i] = (rhs[i] + near[i] * q[last]) * inv
            c[i] = far[i] * inv
            last = i
    i = mid
    inv = 1.0 / (diag[i] - low[i] * c[i - 1] - up[i] * c[i + 1])
    q[i] = (rhs[i] + low[i] * q[i - 1] + up[i] * q[i + 1]) * inv
    for i in range(mid - 1, -1, -1):
        q[i] = q[i] + c[i] * q[i + 1]
    for i in range(mid + 1, n):
        q[i] = q[i] + c[i] * q[i - 1]
    return q


def shift_order(group):
    return [1, 3, 2, 0]


def across_order(group):
    return [1, 2, 3, 0]


def system(blocks, nothing):
    low, diag, up, rhs = [], [], [], []
    for before, after in zip([nothing] + blocks, blocks + [nothing]):
        e = 0.5 * (before[6] + after[5])
        low.append(e * before[1])
        diag.append(1.0 + e * (before[2] + after[0]))
        up.append(e * after[1])
        rhs.append(e * (after[3] - before[4]))
    return low, diag, up, rhs


def merge_kernel(group, *refs):
    got, sup, inner, recv = refs[:group], refs[group], refs[group + 1], refs[group + 2]
    own = sup.shape[0] // 7
    mine = lax.rem(lax.axis_index("row"), group)
    for step, ref in zip(shift_order(group), got):
        recv[lax.rem(mine + group - step, group)] = ref[...]
    blocks = [tuple(recv[d, q * own : (q + 1) * own, :] for q in range(7)) for d in range(group)]
    low, diag, up, rhs = system(blocks, blocks[0])
    low, diag, up, rhs = low[1:group], diag[1:group], up[1:group], rhs[1:group]
    inv = 1.0 / diag[0]
    c_first, a_first, b_first = up[0] * inv, rhs[0] * inv, low[0] * inv
    inv = 1.0 / diag[2]
    c_last, a_last, g_last = low[2] * inv, rhs[2] * inv, up[2] * inv
    inv = 1.0 / (diag[1] - low[1] * c_first - up[1] * c_last)
    a_mid = (rhs[1] + low[1] * a_first + up[1] * a_last) * inv
    b_mid = low[1] * b_first * inv
    g_mid = up[1] * g_last * inv
    a_first, b_first, g_first = a_first + c_first * a_mid, b_first + c_first * b_mid, c_first * g_mid
    a_last, b_last, g_last = a_last + c_last * a_mid, c_last * b_mid, g_last + c_last * g_mid
    first, last = blocks[0], blocks[group - 1]
    parts = [
        first[0] - first[1] * b_first,
        first[1] * g_first,
        last[2] - last[1] * g_last,
        first[3] + first[1] * a_first,
        last[4] - last[1] * a_last,
        first[5],
        last[6],
    ]
    for q, part in enumerate(parts):
        sup[q * own : (q + 1) * own, :] = part
    kept = [a_first, a_mid, a_last, b_first, b_mid, b_last, g_first, g_mid, g_last]
    for q, part in enumerate(kept):
        inner[q * own : (q + 1) * own, :] = part


def flux_kernel(group, *refs):
    got, inner, sends = refs[:group], refs[group], refs[group + 3 : 2 * group + 3]
    recv, flux, send = refs[2 * group + 3 :]
    own = got[0].shape[0] // 7
    row_index = lax.axis_index("row")
    mine, outer = lax.rem(row_index, group), lax.div(row_index, group)
    for step, ref in zip(across_order(group), got):
        recv[lax.rem(outer + group - step, group)] = ref[...]
    blocks = [tuple(recv[d, q * own : (q + 1) * own, :] for q in range(7)) for d in range(group)]
    q = solve(*system(blocks, (jnp.zeros((own, 128), F32),) * 7))
    for i in range(group + 1):
        flux[i] = q[i]
    left, right = flux[outer], flux[outer + 1]

    def kept(i):
        return inner[i * own : (i + 1) * own, :]

    q = [left]
    for i in range(group - 1):
        q.append(kept(i) + kept(group - 1 + i) * left + kept(2 * group - 2 + i) * right)
    q.append(right)
    for d in range(group):
        send[d, 0:own, :] = q[d]
        send[d, own : 2 * own, :] = q[d + 1]
    for step, out in enumerate(sends):
        out[...] = send[lax.rem(mine + step, group)]


def y_send_kernel(nx, group, *refs):
    got = refs[:group]
    bx, g0x, glx, u, g0, gl, faces, send, dt, ql, qr = refs[group:]
    own = got[0].shape[0] // 2
    ny = dt.shape[0] // 8
    mine = lax.rem(lax.axis_index("row"), group)
    for step, ref in zip(shift_order(group), got):
        start = pl.multiple_of(lax.rem(mine + group - step, group) * own, own)
        ql[pl.ds(start, own), :] = ref[0:own, :]
        qr[pl.ds(start, own), :] = ref[own : 2 * own, :]
    for t in range(8):
        zs = slice(t * 8, t * 8 + 8)
        left, right = ql[zs, :], qr[zs, :]
        turn(
            [
                (bx[i, zs, :] - tile(u, nx, t, i))
                + (glx[i, zs, :] * right - g0x[i, zs, :] * left)
                for i in range(nx)
            ],
            dt,
            t,
        )

    zero = jnp.zeros((8, 128), F32)
    b0, bl = [zero] * 4, [zero] * 4
    for j in range(ny):
        dj = row(dt, j)
        b0[j % 4] = b0[j % 4] + row(g0, j) * dj
        bl[j % 4] = bl[j % 4] + row(gl, j) * dj
    root_left, root_right = faces[0:8, :], faces[8:16, :]
    parts = [
        root_left * root_left * row(g0, 0),
        root_left * root_right * row(g0, ny - 1),
        root_right * root_right * row(gl, ny - 1),
        root_left * ((b0[0] + b0[1]) + (b0[2] + b0[3])),
        root_right * ((bl[0] + bl[1]) + (bl[2] + bl[3])),
    ]
    for q, part in enumerate(parts):
        send[q * 8 : (q + 1) * 8, :] = part


def join_kernel(mine, other, sup, mid):
    even = lax.rem(lax.axis_index("col"), 2) == 0
    first, second = [], []
    for q in range(5):
        here, there = mine[q * 8 : q * 8 + 8, :], other[q * 8 : q * 8 + 8, :]
        first.append(jnp.where(even, here, there))
        second.append(jnp.where(even, there, here))
    inv = 1.0 / (1.0 + (first[2] + second[0]))
    f = (second[3] - first[4]) * inv
    g, h = first[1] * inv, second[1] * inv
    parts = [
        first[0] - first[1] * g,
        first[1] * h,
        second[2] - second[1] * h,
        first[3] + first[1] * f,
        second[4] - second[1] * f,
    ]
    for q, part in enumerate(parts):
        sup[q * 8 : q * 8 + 8, :] = part
    for q, part in enumerate((f, g, h)):
        mid[q * 8 : q * 8 + 8, :] = part


def finish_kernel(nx, steps, *refs):
    peers = len(steps)
    got = refs[:peers]
    mid, b, g0, gl, u, faces, out, recv, flux, whole, done, sems = refs[peers:]
    col = lax.axis_index("col")
    chip = lax.div(col, 2)
    for step, ref in zip(steps, got):
        recv[lax.rem(chip + peers - step, peers)] = ref[...]
    nothing = (jnp.zeros((8, 128), F32),) * 5
    low, diag, up, rhs = [], [], [], []
    before = nothing
    for i in range(peers + 1):
        after = nothing
        if i < peers:
            after = tuple(recv[i, q * 8 : (q + 1) * 8, :] for q in range(5))
        low.append(before[1])
        diag.append(1.0 + (before[2] + after[0]))
        up.append(after[1])
        rhs.append(after[3] - before[4])
        before = after
    q = solve(low, diag, up, rhs)
    for i in range(peers + 1):
        flux[i] = q[i]
    left, right = flux[chip], flux[chip + 1]
    inner = mid[0:8, :] + mid[8:16, :] * left + mid[16:24, :] * right
    even = lax.rem(col, 2) == 0
    left, right = jnp.where(even, left, inner), jnp.where(even, inner, right)
    left = left * faces[0:8, :]
    right = right * faces[8:16, :]
    for j in range(b.shape[0] // 8):
        put(whole, j, row(b, j) + (row(gl, j) * right - row(g0, j) * left))
    copies = []
    for i in range(8):
        delta = turn_back(whole, i)
        for x in range(nx):
            done[pl.ds(i * 128 + x, 8, stride=nx), :] = delta[x * 8 : x * 8 + 8, :]
        span = slice(i * 128, (i + 1) * 128)
        done[span, :] = u[span, :] + done[span, :]
        rows = pl.ds(i * 128, 128)
        copy = pltpu.make_async_copy(done.at[rows], out.at[rows], sems.at[i])
        copy.start()
        copies.append(copy)
    for copy in copies:
        copy.wait()


def on_device(field, conductivity):
    nz, nx, ny = field.shape
    rows = nz * nx
    rowp, colp = lax.axis_size("row"), lax.axis_size("col")
    u = field.reshape(rows, ny)
    k = conductivity.reshape(rows, ny)
    flat, cube = (rows, ny), (nx, nz, ny)
    uv, kv, ut, kt, low, high = call(
        functools.partial(load_kernel, nx),
        [flat] * 4 + [(16, 128)] * 2,
        tuple(pltpu.with_memory_space_constraint(a, pltpu.HBM) for a in (u, k)),
        1 << 20,
        [pltpu.SemaphoreType.DMA((2,))],
        [HBM, HBM],
    )
    up = [(i, (i + 1) % colp) for i in range(colp)]
    from_left = lax.ppermute(high, "col", up)
    from_right = lax.ppermute(low, "col", [(b, a) for a, b in up])
    mx, px, g0x, glx, r, ends = call(
        functools.partial(pivots_kernel, nx),
        [cube] * 4 + [flat, (2, nz, ny)],
        (uv, kv, ut, kt),
        1 << 23,
        [flat, flat],
    )
    group = math.isqrt(rowp)
    own = nz // group
    inside, across = {}, {}
    for step in range(group):
        inside[step] = [
            (i * colp + c, (i // group * group + (i + step) % group) * colp + (c ^ 1))
            for i in range(rowp)
            for c in range(colp)
        ]
        across[step] = [(i, (i + step * group) % rowp) for i in range(rowp)]

    def exchange(arrays, pairs, axes):
        return [
            lax.ppermute(arrays[step], axes, pairs[step]) if step or axes != "row" else arrays[0]
            for step in (across_order if axes == "row" else shift_order)(group)
        ]

    *parts, full, faces = call(
        functools.partial(x_send_kernel, nx, colp, group),
        [(7 * own, ny)] * group + [flat, (16, 128)],
        (low, high, from_left, from_right, r, ends, g0x, glx),
        1 << 22,
        [(128, 128), (group, 7 * own, ny)],
    )
    parts = exchange(parts, inside, ("row", "col"))
    (bx,) = call(functools.partial(x_inner_kernel, nx), [cube], (full, mx, px), 1 << 21)
    g0y, gly = call(functools.partial(y_columns_kernel, nx), [flat] * 2, (k,), 1 << 23, [flat] * 3)
    merged, inner = call(
        functools.partial(merge_kernel, group),
        [(7 * own, ny), (9 * own, ny)],
        parts,
        1 << 20,
        [(group, 7 * own, ny)],
    )
    parts = exchange([merged] * group, across, "row")
    parts = call(
        functools.partial(flux_kernel, group),
        [(2 * own, ny)] * group,
        (*parts, inner, bx, g0y),
        1 << 20,
        [(group, 7 * own, ny), (group + 1, own, ny), (group, 2 * own, ny)],
    )
    parts = exchange(parts, inside, ("row", "col"))
    send, dt = call(
        functools.partial(y_send_kernel, nx, group),
        [(40, 128), flat],
        (*parts, bx, g0x, glx, u, g0y, gly, faces),
        1 << 22,
        [(nz, ny), (nz, ny)],
    )
    my, py = call(functools.partial(y_pivots_kernel, nx), [flat] * 2, (k, send), 1 << 22, [flat])
    (b,) = call(y_inner_kernel, [flat], (dt, my, py), 1 << 22)
    other = lax.ppermute(send, "col", [(i, i ^ 1) for i in range(colp)])
    sup, mid = call(join_kernel, [(40, 128), (24, 128)], (send, other), 1 << 16)
    chips = colp // 2
    steps = [0, 2, 1, 3]
    got = [
        lax.ppermute(sup, "col", [(i, (i + 2 * step) % colp) for i in range(colp)]) if step else sup
        for step in steps
    ]
    (out,) = call(
        functools.partial(finish_kernel, nx, steps),
        [flat],
        (*got, mid, b, g0y, gly, u, faces),
        1 << 22,
        [(chips, 40, 128), (chips + 1, 8, 128), flat, flat, pltpu.SemaphoreType.DMA((8,))],
        out_specs=[HBM],
    )
    return out.reshape(nz, nx, ny)


def solution(mesh):
    in_specs = (P(None, "row", "col"), P(None, "row", "col"))
    out_specs = P(None, "row", "col")
    return jax.shard_map(
        on_device, mesh=mesh, in_specs=in_specs, out_specs=out_specs, check_vma=False
    )
```
